32 devices in a mesh: groups: 2 (over y), seq: 4 (over z), tensor: 2 (over x), cfg: 2 (over core).
Axes of the slice: x: 2, y: 2, z: 4, core: 2. Of those that a mesh axis runs over, the one named last changes fastest.
Arguments:
- latent: bfloat16 [2048, 3072], P(('groups', 'seq')), parts along dimension 0, may hold values from -6 to 6
- positions: int32 [3, 2048], P(None, ('groups', 'seq')), parts along dimension 1, may hold values from 0 to 79, as said below
- text_kv: bfloat16 [2, 2, 128, 3072], P('cfg', None, ('groups', 'seq'), 'tensor'), parts along dimension 2, may hold values from -6 to 6
- text_len: int32 [4], P(('groups', 'cfg')), parts along dimension 0, may hold values from 1 to 64
- modulation: float32 [3, 4, 3072], P(None, 'groups'), parts along dimension 1, may hold values from -3 to 3
- w_qkv: bfloat16 [3, 3072, 3072], P(None, 'cfg', 'tensor'), may hold values from -0.109375 to 0.109375
- norm_gains: float32 [2, 128], replicated, may hold values from 0.5 to 2.5
- w_out: bfloat16 [3072, 3072], P('tensor', 'cfg'), may hold values from -0.109375 to 0.109375
- guidance: float32 [2], P('groups'), parts along dimension 0, may hold values from 3 to 8
Outputs:
- guided: bfloat16 [2048, 3072], P(('groups', 'seq', 'tensor'), 'cfg'), parts along dimension 0
The draws below stay inside these ranges and needn't reach their ends.
There are 2 independent parts, one for each index of `groups`. The reference program is written for one: setup_inputs(seed, part) draws one part's arguments, and reference() takes and returns one part's arrays. A program takes and returns all parts, laid end to end along the dimension named above; an argument that names none is the same for every part. Nothing has to cross between parts.
Inputs may be any that keep to these rules, and one draw needn't show every extreme that they name: `positions`: frame indices are below 33, height indices below 45, width indices below 80. `text_len`: text rows at or beyond the count are ignored.
All inputs are finite; a program needn't handle non-finite values.
Results may differ from the reference program's by a relative error of at most 0.018.
Values may be sent and summed in bfloat16 or wider, within the bound.
A program may use at most 128 MiB of HBM per device.

```python
import math
import jax
import jax.numpy as jnp
from jax import lax

D = 3072
HEADS = 24
HEAD_DIM = 128
TOKENS = 1024
TEXT = 64


def draw_positions(key, part):
    keys = jax.random.split(jax.random.fold_in(key, 11), 3)
    frame = jax.random.randint(keys[0], (TOKENS,), 0, 33)
    height = jax.random.randint(keys[1], (TOKENS,), 0, 45)
    across = jax.random.randint(keys[2], (TOKENS,), 0, 80)
    return jnp.stack([frame, height, across]).astype(jnp.int32)


def level_of(stream_key, extent, cuts, smallest, largest):
    level, own = 1.0, jax.random.fold_in(stream_key, 6)
    for dim, shards_of in cuts:
        heights = jnp.exp(jax.random.uniform(jax.random.fold_in(own, dim), (shards_of,), jnp.float32, smallest / len(cuts), largest / len(cuts)))
        level = level * jnp.repeat(heights, extent[dim] // shards_of).reshape([-1 if axis == dim else 1 for axis in range(len(extent))])
    return level


def normal_values(stream_key, extent, scale, bound, cuts=(), kind=jnp.bfloat16):
    entries = jax.random.normal(stream_key, extent, jnp.float32) * scale
    if len(cuts) > 0:
        entries = level_of(stream_key, extent, cuts, -0.22, 0.18) * entries
    return jnp.clip(entries, min=-bound, max=bound).astype(kind)


def setup_inputs(seed: int = 0, part: int = 0) -> dict:
    splits = jax.random.split(jax.random.key(seed), 10)
    own_keys = jax.random.split(jax.random.fold_in(splits[9], part), 10)
    return {
        "latent": normal_values(own_keys[0], (TOKENS, D), 1.0, 6.0, ((0, 4),)),
        "positions": draw_positions(jax.random.fold_in(jax.random.fold_in(splits[9], part), 71), part),
        "text_kv": normal_values(own_keys[2], (2, 2, TEXT, D), 1.0, 6.0, ((0, 2), (2, 4), (3, 2))),
        "text_len": jax.random.randint(own_keys[3], (2,), 1, TEXT + 1).astype(jnp.int32),
        "modulation": normal_values(own_keys[4], (3, 2, D), 0.5, 3.0, (), jnp.float32),
        "w_qkv": normal_values(splits[5], (3, D, D), D ** -0.5, 0.109375, ((1, 2), (2, 2))),
        "norm_gains": jnp.clip(jnp.exp(jax.random.uniform(splits[6], (2, HEAD_DIM), jnp.float32, math.log(0.5), math.log(2.5))), 0.5, 2.5),
        "w_out": normal_values(splits[7], (D, D), D ** -0.5, 0.109375, ((0, 2), (1, 2))),
        "guidance": jnp.clip(jax.random.uniform(own_keys[8], (1,), jnp.float32, 3.0, 8.0), 3.0, 8.0),
    }


def head_norm(heads_in, gain):
    return heads_in * lax.rsqrt(lax.optimization_barrier(jnp.mean(heads_in * heads_in, axis=-1, keepdims=True)) + 1e-06) * gain

def rotary(heads_in, positions):
    head_size = heads_in.shape[-1]
    blocks = (head_size // 8, 7 * head_size // 16, 7 * head_size // 16)
    pieces = []
    offset = 0
    for axis_id in range(3):
        width = blocks[axis_id]
        half = width // 2
        freq = 256.0 ** (-jnp.arange(half, dtype=jnp.float32) / half)
        angle = positions[axis_id].astype(jnp.float32)[:, None] * freq[None, :]
        cosine = jnp.cos(angle)[:, None, :]
        sine = jnp.sin(angle)[:, None, :]
        first = heads_in[..., offset:offset + half]
        second = heads_in[..., offset + half:offset + width]
        pieces.append(first * cosine - second * sine)
        pieces.append(second * cosine + first * sine)
        offset = offset + width
    return jnp.concatenate(pieces, axis=-1)

def reference(latent, positions, text_kv, text_len, modulation, w_qkv, norm_gains, w_out, guidance):
    rows = latent.shape[0]
    xfloat = latent.astype(jnp.float32)
    center = xfloat - lax.optimization_barrier(jnp.mean(xfloat, axis=-1, keepdims=True))
    normed = center * lax.rsqrt(lax.optimization_barrier(jnp.mean(center * center, axis=-1, keepdims=True)) + 1e-06)
    scale = HEAD_DIM ** (-0.5)
    outputs = []
    for branch in range(2):
        modulated = (normed * (1.0 + modulation[1, branch]) + modulation[0, branch]).astype(jnp.bfloat16)
        projected = [jnp.dot(modulated, w_qkv[j], preferred_element_type=jnp.float32) for j in range(3)]
        queries = rotary(head_norm(projected[0].reshape(rows, HEADS, HEAD_DIM), norm_gains[0]), positions).astype(jnp.bfloat16)
        keys = rotary(head_norm(projected[1].reshape(rows, HEADS, HEAD_DIM), norm_gains[1]), positions).astype(jnp.bfloat16)
        value_rows = projected[2].astype(jnp.bfloat16).reshape(rows, HEADS, HEAD_DIM)
        prompt_keys = head_norm(text_kv[branch, 0].astype(jnp.float32).reshape(TEXT, HEADS, HEAD_DIM), norm_gains[1]).astype(jnp.bfloat16)
        all_keys = jnp.concatenate([keys, prompt_keys], axis=0)
        all_values = jnp.concatenate([value_rows, text_kv[branch, 1].reshape(TEXT, HEADS, HEAD_DIM)], axis=0)
        valid = jnp.concatenate([jnp.ones((rows,), bool), jnp.arange(TEXT, dtype=jnp.int32) < text_len[branch]])

        def one_head(operands):
            query_head, key_head, value_head = operands
            scores = jnp.dot(query_head, key_head.T, preferred_element_type=jnp.float32) * scale
            expo = jnp.where(valid[None, :], jnp.exp(scores), 0.0)
            total = lax.optimization_barrier(jnp.sum(expo, axis=-1, keepdims=True))
            mixed = jnp.dot(expo.astype(jnp.bfloat16), value_head, preferred_element_type=jnp.float32)
            return mixed / total
        attended = lax.map(one_head, (queries.transpose(1, 0, 2), all_keys.transpose(1, 0, 2), all_values.transpose(1, 0, 2)))
        attended = attended.transpose(1, 0, 2).reshape(rows, HEADS * HEAD_DIM).astype(jnp.bfloat16)
        branch_out = (modulation[2, branch] * jnp.dot(attended, w_out, preferred_element_type=jnp.float32)).astype(jnp.bfloat16)
        outputs.append(lax.optimization_barrier(branch_out).astype(jnp.float32))
    return (outputs[1] + guidance[0] * (outputs[0] - outputs[1])).astype(jnp.bfloat16)
```

```python
import functools

import jax
import jax.numpy as jnp
import numpy as np
from jax import lax
from jax.experimental import pallas as pl
from jax.experimental.pallas import tpu as pltpu
from jax.sharding import PartitionSpec as P

HEAD_DIM = 128
MESH = pl.DeviceIdType.MESH
U_TILE = True
U_MOD = 8
U_ATT = 4
U_TEXT = 2
F32 = jnp.float32
BF16 = jnp.bfloat16


def rotary_rows(head_size):
    rows = np.zeros((8, head_size), np.float32)
    axes = np.zeros((head_size,), np.int32)
    blocks = (head_size // 8, 7 * head_size // 16, 7 * head_size // 16)
    halves = []
    offset = 0
    for axis_id, width in enumerate(blocks):
        half = width // 2
        if half not in halves:
            halves.append(half)
        which = halves.index(half)
        freq = (256.0 ** (-np.arange(half, dtype=np.float64) / half)).astype(np.float32)
        rows[0, offset : offset + half] = freq
        rows[0, offset + half : offset + width] = freq
        rows[1 + 2 * which, offset : offset + half] = -1.0
        rows[2 + 2 * which, offset + half : offset + width] = 1.0
        axes[offset : offset + width] = axis_id
        offset += width
    shifts = []
    for half in halves:
        shifts += [head_size - half, half]
    return rows, axes, tuple(shifts)


ROT_ROWS, ROT_AXES, ROT_SHIFTS = rotary_rows(HEAD_DIM)
ROT_PICK = (np.arange(16)[:, None] == ROT_AXES[None, :]).astype(np.float32)


STRIP = 16


def kernel(
    seq_n,
    ten_n,
    latent,
    pos_in,
    text_kv,
    lens_in,
    modulation,
    w_qkv,
    gains,
    w_out,
    guide,
    rot,
    pick,
    out,
    lat,
    pos,
    txt,
    txo,
    lens,
    wfull,
    wout,
    mod,
    tab,
    qbuf,
    kbuf,
    vbuf,
    acc,
    lsum,
    attf,
    part,
    got,
    send_a,
    recv_a,
    send_b,
    recv_b,
    send_c,
    recv_c,
    send_p,
    recv_p,
    send_t,
    recv_t,
    send_u,
    recv_u,
    send_w,
    recv_w,
    send_l,
    recv_l,
    send_o,
    recv_o,
    send_r,
    recv_r,
    loc,
):
    x = lax.axis_index("tensor")
    c = lax.axis_index("cfg")
    z = lax.axis_index("seq")
    other = 1 - c
    rows, width = latent.shape
    half = w_qkv.shape[1]
    mine = wfull.shape[2]
    heads = mine // HEAD_DIM
    half_rows = rows // 2
    band = ten_n * STRIP
    subs = half_rows // band
    out_rows = rows // ten_n
    out_cols = w_out.shape[1]
    scale = HEAD_DIM ** (-0.5)
    tile = 256 if mine % 256 == 0 else 128
    per_tile = tile // HEAD_DIM
    tiles = mine // tile
    shorter = jnp.minimum(z, seq_n - 1 - z)
    long_sign = jnp.where(2 * z < seq_n - 1, 1, -1)

    def order(i):
        near = i <= 2 * shorter
        dist = jnp.where(near, (i + 1) // 2, i - shorter)
        sign = jnp.where(near, 2 * (i % 2) - 1, long_sign)
        return jnp.where(i == 0, z, z + dist * sign)

    def remote(src, dst, send, recv, **to):
        return pltpu.make_async_remote_copy(
            src_ref=src, dst_ref=dst, send_sem=send, recv_sem=recv, device_id=to, device_id_type=MESH
        )

    def aligned(value, unit):
        return pl.multiple_of(value * unit, unit)

    def inside(o):
        return jnp.logical_and(o >= 0, o < seq_n)

    cols_of = lambda core: pl.ds(aligned(core, mine), mine)
    w_copy = [
        remote(
            w_qkv.at[j, :, cols_of(other)],
            wfull.at[j, pl.ds(aligned(c, half), half), :],
            send_w.at[j],
            recv_w.at[j],
            cfg=other,
        )
        for j in range(3)
    ]
    w_local = [
        pltpu.make_async_copy(
            w_qkv.at[j, :, cols_of(c)], wfull.at[j, pl.ds(aligned(c, half), half), :], loc.at[j]
        )
        for j in range(3)
    ]
    lat_local = pltpu.make_async_copy(latent, lat.at[z], loc.at[3])
    pos_local = pltpu.make_async_copy(pos_in, pos.at[z], loc.at[4])
    txt_local = pltpu.make_async_copy(text_kv.at[0], txt.at[z], loc.at[5])
    len_local = pltpu.make_async_copy(lens_in, lens.at[c], loc.at[6])
    out_local = pltpu.make_async_copy(w_out, wout, loc.at[7])

    def strip_of(core, s, ten):
        return pl.ds(aligned((core * subs + s) * ten_n + ten, STRIP), STRIP)

    def band_of(core, s):
        return pl.ds(aligned(core * subs + s, band), band)

    def up(d):
        return 0 if d > 0 else 1

    def first_a(s, d):
        at = strip_of(c, s, x)
        return remote(latent.at[at], lat.at[z, at], send_a.at[z, s, up(d)], recv_a.at[z, s], seq=z + d)

    def copy_a(o, s, d):
        at = strip_of(c, s, x)
        return remote(lat.at[o, at], lat.at[o, at], send_a.at[o, s, up(d)], recv_a.at[o, s], seq=z + d)

    def copy_b(o, s, t):
        at = strip_of(c, s, x)
        to = (x + t) % ten_n
        return remote(lat.at[o, at], lat.at[o, at], send_b.at[o, s, t], recv_b.at[o, s, t], tensor=to)

    def arrived_b(o, s, t):
        source = (x + ten_n - t) % ten_n
        at = strip_of(c, s, source)
        return remote(lat.at[o, at], lat.at[o, at], send_b.at[o, s, t], recv_b.at[o, s, t], tensor=source)

    def copy_c(o, s, core):
        at = band_of(core, s)
        return remote(lat.at[o, at], lat.at[o, at], send_c.at[o, s], recv_c.at[o, s], cfg=other)

    def first_p(d):
        return remote(pos_in, pos.at[z], send_p.at[z, up(d)], recv_p.at[z], seq=z + d)

    def copy_p(o, d):
        return remote(pos.at[o], pos.at[o], send_p.at[o, up(d)], recv_p.at[o], seq=z + d)

    def first_t(d):
        return remote(text_kv.at[0], txt.at[z], send_t.at[z, up(d)], recv_t.at[z], seq=z + d)

    def copy_t(o, d):
        return remote(txt.at[o], txt.at[o], send_t.at[o, up(d)], recv_t.at[o], seq=z + d)

    def first_u():
        return remote(
            text_kv.at[0, :, :, cols_of(other)], txo.at[z], send_u.at[z], recv_u.at[z], cfg=other
        )

    def copy_u(o):
        return remote(txt.at[o, :, :, cols_of(other)], txo.at[o], send_u.at[o], recv_u.at[o], cfg=other)

    def copy_l(core):
        return remote(lens_in, lens.at[core], send_l.at[0], recv_l.at[0], cfg=other)

    for j in range(3):
        w_local[j].start()
    lat_local.start()
    pos_local.start()
    txt_local.start()
    len_local.start()
    out_local.start()

    barrier = pltpu.get_barrier_semaphore()
    for d in (1, -1):

        @pl.when(inside(z + d))
        def _():
            pl.semaphore_signal(barrier, inc=1, device_id={"seq": z + d}, device_id_type=MESH)

    pl.semaphore_signal(barrier, inc=1, device_id={"cfg": other}, device_id_type=MESH)
    for t in range(1, ten_n):
        pl.semaphore_signal(
            barrier, inc=1, device_id={"tensor": (x + t) % ten_n}, device_id_type=MESH
        )
    sides = jnp.where(z > 0, 1, 0) + jnp.where(z < seq_n - 1, 1, 0)
    pl.semaphore_wait(barrier, ten_n + sides)

    for d in (1, -1):

        @pl.when(inside(z + d))
        def _():
            first_p(d).start()
            for s in range(subs):
                first_a(s, d).start()

    for j in range(3):
        w_copy[j].start()
    copy_l(c).start()
    first_u().start()
    for d in (1, -1):

        @pl.when(inside(z + d))
        def _():
            first_t(d).start()

    acc[...] = jnp.zeros_like(acc)
    lsum[...] = jnp.zeros_like(lsum)
    lat_local.wait()
    pos_local.wait()

    def pump_a(k, s):
        for d in (1, -1):
            o = z - d * k

            @pl.when(inside(o))
            def _():
                if s == 0:
                    copy_p(o, d).wait_recv()
                copy_a(o, s, d).wait_recv()

                @pl.when(inside(z + d))
                def _():
                    if s == 0:
                        copy_p(o, d).start()
                    copy_a(o, s, d).start()

    def pump_t(k):
        for d in (1, -1):
            o = z - d * k

            @pl.when(inside(o))
            def _():
                copy_t(o, d).wait_recv()

                @pl.when(inside(z + d))
                def _():
                    copy_t(o, d).start()

                copy_u(o).start()

    def start_b(o, s):
        for t in range(1, ten_n):
            copy_b(o, s, t).start()

    def end_b(o, s):
        for t in range(1, ten_n):
            arrived_b(o, s, t).wait_recv()
        copy_c(o, s, c).start()

    slots = 2 * tiles + 3

    def pump(i, slot):
        @pl.when(i + 1 < seq_n)
        def _():
            o = order(i + 1)
            for s in range(subs):
                if slot == min(2 * s, slots - 3):
                    pump_a(i + 1, s)
                    start_b(o, s)
            for s in range(subs):
                if slot == min(2 * s + 1, slots - 2):
                    end_b(o, s)
            if slot == slots - 2:
                pump_t(i + 1)

    def normed_head(value, gain):
        return (
            value * lax.rsqrt(jnp.mean(value * value, axis=-1, keepdims=True) + 1e-06) * gain
        )

    def turned(value):
        total = value * tab[0]
        for k, shift in enumerate(ROT_SHIFTS):
            total = total + pltpu.roll(value, shift, 1) * tab[1 + k]
        return total

    def project(j, t):
        at = pl.ds(t * tile, tile)
        return [
            jnp.dot(mod[b * rows : (b + 1) * rows, :], wfull[j, :, at], preferred_element_type=F32)
            for b in range(2)
        ]

    def head_tile(j, gain_row, dest, t):
        y = project(j, t)
        gain = gains[gain_row : gain_row + 1, :]
        for hh in range(per_tile):
            for b in range(2):
                part_in = y[b][:, hh * HEAD_DIM : (hh + 1) * HEAD_DIM]
                dest[b * heads + t * per_tile + hh] = turned(normed_head(part_in, gain)).astype(BF16)

    def value_tile(t):
        y = [value.astype(BF16) for value in project(2, t)]
        for hh in range(per_tile):
            for b in range(2):
                vbuf[b * heads + t * per_tile + hh] = y[b][:, hh * HEAD_DIM : (hh + 1) * HEAD_DIM]

    def attend(h):
        scores = lax.dot_general(
            qbuf[h], kbuf[h], (((1,), (1,)), ((), ())), preferred_element_type=F32
        )
        expo = jnp.exp(scores * scale)
        folded = expo[:, :HEAD_DIM]
        for k in range(1, rows // HEAD_DIM):
            folded = folded + expo[:, k * HEAD_DIM : (k + 1) * HEAD_DIM]
        lsum[h] += folded
        acc[h] += jnp.dot(expo.astype(BF16), vbuf[h], preferred_element_type=F32)

    @pl.loop(0, seq_n)
    def _(i):
        o = order(i)

        @pl.when(i > 0)
        def _():
            for s in range(subs):
                copy_c(o, s, other).wait_recv()

        place = lax.dot_general(
            pos[o], pick[...], (((0,), (0,)), ((), ())), preferred_element_type=F32
        )
        angle = place * rot[0:1, :]
        sine = jnp.sin(angle)
        tab[0] = jnp.cos(angle)
        for k in range(len(ROT_SHIFTS)):
            tab[1 + k] = sine * rot[1 + k : 2 + k, :]

        @pl.loop(0, rows // STRIP, unroll=U_MOD)
        def _(r):
            at = pl.ds(pl.multiple_of(r * STRIP, STRIP), STRIP)
            value = lat[o, at, :].astype(F32)
            center = value - jnp.mean(value, axis=-1, keepdims=True)
            normed = center * lax.rsqrt(jnp.mean(center * center, axis=-1, keepdims=True) + 1e-06)
            for b in range(2):
                mod[pl.ds(pl.multiple_of(b * rows + r * STRIP, STRIP), STRIP), :] = (
                    normed * (1.0 + modulation[1, b : b + 1, :]) + modulation[0, b : b + 1, :]
                ).astype(BF16)

        @pl.when(i == 0)
        def _():
            w_local[0].wait()
            w_copy[0].wait_recv()
            for t in range(tiles):
                head_tile(0, 0, qbuf, t)
            w_local[1].wait()
            w_copy[1].wait_recv()

        for t in range(tiles):
            head_tile(1, 1, kbuf, t)
            pump(i, t)

        @pl.when(i == 0)
        def _():
            w_local[2].wait()
            w_copy[2].wait_recv()

        for t in range(tiles):
            value_tile(t)
            pump(i, tiles + t)

        group = (2 * heads + 2) // 3
        for g in range(3):

            @pl.loop(g * group, min((g + 1) * group, 2 * heads), unroll=True)
            def _(h):
                attend(h)

            pump(i, 2 * tiles + g)

    txt_local.wait()
    len_local.wait()
    copy_l(other).wait_recv()

    @pl.loop(0, seq_n)
    def _(o):
        copy_u(o).wait_recv()

    text_rows = txt.shape[2]
    count = seq_n * text_rows

    def copy_o(core, branch):
        return remote(
            attf.at[core, branch], attf.at[core, branch], send_o.at[branch], recv_o.at[branch], cfg=other
        )

    for own in range(2):
        branch = c if own == 0 else other
        source = txt if own == 0 else txo
        base = aligned(c, mine) if own == 0 else 0
        valid = lax.broadcasted_iota(jnp.int32, (1, count), 1).astype(F32) < lens[branch, 0:1, :]

        @pl.loop(0, heads, unroll=U_TEXT)
        def _(h):
            at = pl.ds(pl.multiple_of(h * HEAD_DIM, HEAD_DIM), HEAD_DIM)
            src = pl.ds(pl.multiple_of(base + h * HEAD_DIM, HEAD_DIM), HEAD_DIM)
            raw = source[:, 0, :, src].reshape(count, HEAD_DIM).astype(F32)
            keys = normed_head(raw, gains[1:2, :]).astype(BF16)
            values = source[:, 1, :, src].reshape(count, HEAD_DIM)
            n = branch * heads + h
            scores = lax.dot_general(
                qbuf[n], keys, (((1,), (1,)), ((), ())), preferred_element_type=F32
            )
            expo = jnp.where(valid, jnp.exp(scores * scale), 0.0)
            total = jnp.sum(lsum[n], axis=-1, keepdims=True) + jnp.sum(
                expo, axis=-1, keepdims=True
            )
            mixed = acc[n] + jnp.dot(expo.astype(BF16), values, preferred_element_type=F32)
            attf[c, branch, :, at] = (mixed / total).astype(BF16)

        copy_o(c, branch).start()

    out_local.wait()
    copy_o(other, other).wait_recv()
    copy_o(other, c).wait_recv()

    out_tile = 256 if out_cols % 256 == 0 else 128
    out_tiles = out_cols // out_tile

    def copy_r(t, k):
        return remote(
            part.at[t, k], got.at[t, k], send_r.at[t, k], recv_r.at[t, k], tensor=(x + t) % ten_n
        )

    def out_block(t, k):
        to = (x + t) % ten_n
        here = pl.ds(pl.multiple_of(to * out_rows, out_rows), out_rows)
        at = pl.ds(pl.multiple_of(k * out_tile, out_tile), out_tile)
        total = None
        strength = guide[0:1, 0:1]
        at_gate = pl.ds(pl.multiple_of(c * out_cols + k * out_tile, out_tile), out_tile)
        gates = (
            strength * modulation[2, 0:1, at_gate],
            (1.0 - strength) * modulation[2, 1:2, at_gate],
        )
        for b in range(2):
            y = jnp.dot(attf[0, b, here, :], wout[0:mine, at], preferred_element_type=F32)
            y = y + jnp.dot(
                attf[1, b, here, :], wout[mine : 2 * mine, at], preferred_element_type=F32
            )
            y = y * gates[b]
            total = y if total is None else total + y
        return total

    for t in range(1, ten_n):

        @pl.loop(0, out_tiles)
        def _(k):
            part[t, k] = out_block(t, k).astype(BF16)
            copy_r(t, k).start()

    @pl.loop(0, out_tiles)
    def _(k):
        part[0, k] = out_block(0, k).astype(BF16)

    for k in range(out_tiles):
        total = part[0, k].astype(F32)
        for t in range(1, ten_n):
            copy_r(t, k).wait_recv()
            total = total + got[t, k].astype(F32)
        out[:, k * out_tile : (k + 1) * out_tile] = total.astype(BF16)

    for j in range(3):
        w_copy[j].wait_send()
    copy_l(c).wait_send()
    for b in range(2):
        copy_o(c, b).wait_send()
    for t in range(1, ten_n):
        for k in range(out_tiles):
            copy_r(t, k).wait_send()

    @pl.loop(0, seq_n)
    def _(o):
        copy_u(o).wait_send()

        @pl.when(o != z)
        def _():
            for s in range(subs):
                for t in range(1, ten_n):
                    copy_b(o, s, t).wait_send()
                copy_c(o, s, c).wait_send()

        for d in (1, -1):
            ahead = jnp.logical_or(o == z, d * (z - o) > 0)

            @pl.when(jnp.logical_and(ahead, inside(z + d)))
            def _():
                copy_p(o, d).wait_send()
                copy_t(o, d).wait_send()
                for s in range(subs):
                    copy_a(o, s, d).wait_send()


def local(
    seq_n, ten_n, latent, positions, text_kv, text_len, modulation, w_qkv, norm_gains, w_out, guidance
):
    rows, width = latent.shape
    mine = w_qkv.shape[2] // 2
    heads = mine // HEAD_DIM
    text_dev = text_kv.shape[2]
    out_rows = rows // ten_n
    out_cols = w_out.shape[1]
    out_tile = 256 if out_cols % 256 == 0 else 128
    out_tiles = out_cols // out_tile
    subs = rows // (2 * ten_n * STRIP)
    pos_in = jnp.pad(positions.astype(BF16), ((0, 13), (0, 0)))
    lens = jnp.broadcast_to(text_len.astype(F32)[None, :], (8, seq_n * text_dev))
    any_space = pl.BlockSpec(memory_space=pl.ANY)
    vmem = pl.BlockSpec(memory_space=pltpu.VMEM)
    dma = pltpu.SemaphoreType.DMA
    return pl.pallas_call(
        functools.partial(kernel, seq_n, ten_n),
        out_shape=jax.ShapeDtypeStruct((out_rows, out_cols), BF16),
        in_specs=[
            any_space,
            any_space,
            any_space,
            any_space,
            vmem,
            any_space,
            vmem,
            any_space,
            vmem,
            vmem,
            vmem,
        ],
        out_specs=vmem,
        scratch_shapes=[
            pltpu.VMEM((seq_n, rows, width), BF16),
            pltpu.VMEM((seq_n, 16, rows), BF16),
            pltpu.VMEM((seq_n, 2, text_dev, 2 * mine), BF16),
            pltpu.VMEM((seq_n, 2, text_dev, mine), BF16),
            pltpu.VMEM((2, 8, seq_n * text_dev), F32),
            pltpu.VMEM((3, width, mine), BF16),
            pltpu.VMEM(w_out.shape, BF16),
            pltpu.VMEM((2 * rows, width), BF16),
            pltpu.VMEM((1 + len(ROT_SHIFTS), rows, HEAD_DIM), F32),
            pltpu.VMEM((2 * heads, rows, HEAD_DIM), BF16),
            pltpu.VMEM((2 * heads, rows, HEAD_DIM), BF16),
            pltpu.VMEM((2 * heads, rows, HEAD_DIM), BF16),
            pltpu.VMEM((2 * heads, rows, HEAD_DIM), F32),
            pltpu.VMEM((2 * heads, rows, HEAD_DIM), F32),
            pltpu.VMEM((2, 2, rows, mine), BF16),
            pltpu.VMEM((ten_n, out_tiles, out_rows, out_tile), BF16),
            pltpu.VMEM((ten_n, out_tiles, out_rows, out_tile), BF16),
            dma((seq_n, subs, 2)),
            dma((seq_n, subs)),
            dma((seq_n, subs, ten_n)),
            dma((seq_n, subs, ten_n)),
            dma((seq_n, subs)),
            dma((seq_n, subs)),
            dma((seq_n, 2)),
            dma((seq_n,)),
            dma((seq_n, 2)),
            dma((seq_n,)),
            dma((seq_n,)),
            dma((seq_n,)),
            dma((3,)),
            dma((3,)),
            dma((1,)),
            dma((1,)),
            dma((2,)),
            dma((2,)),
            dma((ten_n, out_tiles)),
            dma((ten_n, out_tiles)),
            dma((8,)),
        ],
        compiler_params=pltpu.CompilerParams(
            collective_id=0, has_side_effects=True, vmem_limit_bytes=64 * 1024 * 1024 - 65536
        ),
    )(
        latent,
        pos_in,
        text_kv,
        lens,
        modulation,
        w_qkv,
        norm_gains,
        w_out,
        guidance.reshape(1, 1),
        jnp.asarray(ROT_ROWS),
        jnp.asarray(ROT_PICK, BF16),
    )


def solution(mesh):
    placed = (
        P(("groups", "seq"), None),
        P(None, ("groups", "seq")),
        P("cfg", None, ("groups", "seq"), "tensor"),
        P(("groups", "cfg")),
        P(None, "groups", None),
        P(None, "cfg", "tensor"),
        P(),
        P("tensor", "cfg"),
        P("groups"),
    )
    return jax.shard_map(
        functools.partial(local, mesh.shape["seq"], mesh.shape["tensor"]),
        mesh=mesh,
        in_specs=placed,
        out_specs=P(("groups", "seq", "tensor"), "cfg"),
        check_vma=False,
    )
```

```python
import functools
import math

import jax
import jax.numpy as jnp
import numpy as np
from jax import lax
from jax.experimental import pallas as pl
from jax.experimental.pallas import tpu as pltpu
from jax.sharding import PartitionSpec as P

HEAD_DIM = 128
MESH = pl.DeviceIdType.MESH
U_MOD = 8
F32 = jnp.float32
BF16 = jnp.bfloat16


def rotary_rows(head_size):
    rows = np.zeros((8, head_size), np.float32)
    swap = np.zeros((head_size, head_size), np.float32)
    axes = np.zeros((head_size,), np.int32)
    blocks = (head_size // 8, 7 * head_size // 16, 7 * head_size // 16)
    offset = 0
    for axis_id, width in enumerate(blocks):
        half = width // 2
        turns = 256.0 ** (-np.arange(half, dtype=np.float64) / half) / (2 * np.pi)
        rows[0, offset : offset + half] = turns
        rows[0, offset + half : offset + width] = turns
        for k in range(half):
            swap[offset + half + k, offset + k] = -1.0
            swap[offset + k, offset + half + k] = 1.0
        axes[offset : offset + width] = axis_id
        offset += width
    return rows, axes, swap


ROT_ROWS, ROT_AXES, ROT_SWAP = rotary_rows(HEAD_DIM)
ROT_PICK = (np.arange(16)[:, None] == ROT_AXES[None, :]).astype(np.float32)
SIDE = np.kron(np.eye(2), np.ones((HEAD_DIM, HEAD_DIM)))
MIX = np.stack([np.kron(np.eye(2), ROT_SWAP), SIDE / HEAD_DIM]).astype(np.float32)
SIN = tuple((-1.0) ** k / math.factorial(2 * k + 1) for k in range(6))
COS = tuple((-1.0) ** k / math.factorial(2 * k) for k in range(6))
LOG2E = 1.4426950408889634


def horner(terms, value):
    total = terms[-1]
    for term in terms[-2::-1]:
        total = total * value + term
    return total


STRIP = 16


def kernel(
    seq_n,
    ten_n,
    latent,
    pos_in,
    text_kv,
    lens_in,
    modulation,
    w_qkv,
    gains,
    w_out,
    guide,
    rot,
    pick,
    mix,
    out,
    lat,
    pos,
    txt,
    txo,
    lens,
    wfull,
    wout,
    mod,
    tab,
    qbuf,
    kbuf,
    vbuf,
    acc,
    lsum,
    attf,
    part,
    got,
    send_a,
    recv_a,
    send_b,
    recv_b,
    send_c,
    recv_c,
    send_p,
    recv_p,
    send_t,
    recv_t,
    send_u,
    recv_u,
    send_w,
    recv_w,
    send_l,
    recv_l,
    send_o,
    recv_o,
    send_r,
    recv_r,
    loc,
):
    x = lax.axis_index("tensor")
    c = lax.axis_index("cfg")
    z = lax.axis_index("seq")
    other = 1 - c
    rows, width = latent.shape
    half = w_qkv.shape[1]
    mine = wfull.shape[2]
    heads = mine // HEAD_DIM
    half_rows = rows // 2
    band = ten_n * STRIP
    subs = half_rows // band
    out_rows = rows // ten_n
    out_cols = w_out.shape[1]
    scale = HEAD_DIM ** (-0.5) * LOG2E
    tile = 256 if mine % 256 == 0 else 128
    per_tile = tile // HEAD_DIM
    tiles = mine // tile
    shorter = jnp.minimum(z, seq_n - 1 - z)
    long_sign = jnp.where(2 * z < seq_n - 1, 1, -1)

    def order(i):
        near = i <= 2 * shorter
        dist = jnp.where(near, (i + 1) // 2, i - shorter)
        sign = jnp.where(near, 2 * (i % 2) - 1, long_sign)
        return jnp.where(i == 0, z, z + dist * sign)

    def remote(src, dst, send, recv, **to):
        return pltpu.make_async_remote_copy(
            src_ref=src, dst_ref=dst, send_sem=send, recv_sem=recv, device_id=to, device_id_type=MESH
        )

    def aligned(value, unit):
        return pl.multiple_of(value * unit, unit)

    def inside(o):
        return jnp.logical_and(o >= 0, o < seq_n)

    cols_of = lambda core: pl.ds(aligned(core, mine), mine)
    w_copy = [
        remote(
            w_qkv.at[j, :, cols_of(other)],
            wfull.at[j, pl.ds(aligned(c, half), half), :],
            send_w.at[j],
            recv_w.at[j],
            cfg=other,
        )
        for j in range(3)
    ]
    w_local = [
        pltpu.make_async_copy(
            w_qkv.at[j, :, cols_of(c)], wfull.at[j, pl.ds(aligned(c, half), half), :], loc.at[j]
        )
        for j in range(3)
    ]
    lat_local = pltpu.make_async_copy(latent, lat.at[z], loc.at[3])
    pos_local = pltpu.make_async_copy(pos_in, pos.at[z], loc.at[4])
    txt_local = pltpu.make_async_copy(text_kv.at[0], txt.at[z], loc.at[5])
    len_local = pltpu.make_async_copy(lens_in, lens.at[c], loc.at[6])
    out_local = pltpu.make_async_copy(w_out, wout, loc.at[7])

    def strip_of(core, s, ten):
        return pl.ds(aligned((core * subs + s) * ten_n + ten, STRIP), STRIP)

    def band_of(core, s):
        return pl.ds(aligned(core * subs + s, band), band)

    def up(d):
        return 0 if d > 0 else 1

    def copy_a(o, s, d):
        at = strip_of(c, s, x)
        return remote(lat.at[o, at], lat.at[o, at], send_a.at[o, s, up(d)], recv_a.at[o, s], seq=z + d)

    def copy_b(o, s, t):
        at = strip_of(c, s, x)
        to = (x + t) % ten_n
        return remote(lat.at[o, at], lat.at[o, at], send_b.at[o, s, t], recv_b.at[o, s, t], tensor=to)

    def arrived_b(o, s, t):
        source = (x + ten_n - t) % ten_n
        at = strip_of(c, s, source)
        return remote(lat.at[o, at], lat.at[o, at], send_b.at[o, s, t], recv_b.at[o, s, t], tensor=source)

    def copy_c(o, s, core):
        at = band_of(core, s)
        return remote(lat.at[o, at], lat.at[o, at], send_c.at[o, s], recv_c.at[o, s], cfg=other)

    def first_p(d):
        return remote(pos_in, pos.at[z], send_p.at[z, up(d)], recv_p.at[z], seq=z + d)

    def copy_p(o, d):
        return remote(pos.at[o], pos.at[o], send_p.at[o, up(d)], recv_p.at[o], seq=z + d)

    def first_t(d):
        return remote(text_kv.at[0], txt.at[z], send_t.at[z, up(d)], recv_t.at[z], seq=z + d)

    def copy_t(o, d):
        return remote(txt.at[o], txt.at[o], send_t.at[o, up(d)], recv_t.at[o], seq=z + d)

    def first_u():
        return remote(
            text_kv.at[0, :, :, cols_of(other)], txo.at[z], send_u.at[z], recv_u.at[z], cfg=other
        )

    def copy_u(o):
        return remote(txt.at[o, :, :, cols_of(other)], txo.at[o], send_u.at[o], recv_u.at[o], cfg=other)

    def copy_l(core):
        return remote(lens_in, lens.at[core], send_l.at[0], recv_l.at[0], cfg=other)

    for j in range(3):
        w_local[j].start()
    lat_local.start()
    pos_local.start()
    txt_local.start()
    len_local.start()
    out_local.start()

    barrier = pltpu.get_barrier_semaphore()
    for d in (1, -1):

        @pl.when(inside(z + d))
        def _():
            pl.semaphore_signal(barrier, inc=1, device_id={"seq": z + d}, device_id_type=MESH)

    pl.semaphore_signal(barrier, inc=1, device_id={"cfg": other}, device_id_type=MESH)
    for t in range(1, ten_n):
        pl.semaphore_signal(
            barrier, inc=1, device_id={"tensor": (x + t) % ten_n}, device_id_type=MESH
        )

    def normalize(at):
        value = lat[z, at, :].astype(F32)
        center = value - jnp.mean(value, axis=-1, keepdims=True)
        normed = center * lax.rsqrt(jnp.mean(center * center, axis=-1, keepdims=True) + 1e-06)
        lat[z, at, :] = normed.astype(BF16)

    lat_local.wait()
    for s in range(subs):
        normalize(strip_of(c, s, x))

    sides = jnp.where(z > 0, 1, 0) + jnp.where(z < seq_n - 1, 1, 0)
    pl.semaphore_wait(barrier, ten_n + sides)

    for d in (1, -1):

        @pl.when(inside(z + d))
        def _():
            first_p(d).start()
            for s in range(subs):
                copy_a(z, s, d).start()

    for j in range(3):
        w_copy[j].start()
    copy_l(c).start()
    first_u().start()
    for d in (1, -1):

        @pl.when(inside(z + d))
        def _():
            first_t(d).start()

    for t in range(1, ten_n):
        for s in range(subs):
            normalize(strip_of(c, s, (x + t) % ten_n))

    @pl.loop(0, half_rows // STRIP, unroll=4)
    def _(r):
        normalize(pl.ds(aligned(other * (half_rows // STRIP) + r, STRIP), STRIP))

    pos_local.wait()

    def pump_a(k, s):
        for d in (1, -1):
            o = z - d * k

            @pl.when(inside(o))
            def _():
                if s == 0:
                    copy_p(o, d).wait_recv()
                copy_a(o, s, d).wait_recv()

                @pl.when(inside(z + d))
                def _():
                    if s == 0:
                        copy_p(o, d).start()
                    copy_a(o, s, d).start()

    def pump_t(k):
        for d in (1, -1):
            o = z - d * k

            @pl.when(inside(o))
            def _():
                copy_t(o, d).wait_recv()

                @pl.when(inside(z + d))
                def _():
                    copy_t(o, d).start()

                copy_u(o).start()

    def start_b(o, s):
        for t in range(1, ten_n):
            copy_b(o, s, t).start()

    def end_b(o, s):
        for t in range(1, ten_n):
            arrived_b(o, s, t).wait_recv()
        copy_c(o, s, c).start()

    def front(k, p):
        @pl.when(k < seq_n)
        def _():
            for s in range(subs):
                if s * 4 // subs == p:
                    pump_a(k, s)
                    start_b(order(k), s)

    def back(k, p):
        @pl.when(k < seq_n)
        def _():
            for s in range(subs):
                if s * 4 // subs == p:
                    end_b(order(k), s)

    slots = 2 * tiles + 2

    def pump(i, slot):
        if slot == 0:
            front(i + 1, 2)
        if slot == 1:
            front(i + 1, 3)
        if slot == tiles:
            back(i + 1, 0)
        if slot == 2 * tiles - 1:
            back(i + 1, 1)

            @pl.when(i + 1 < seq_n)
            def _():
                pump_t(i + 1)

        if slot == 2 * tiles:
            back(i + 1, 2)
            front(i + 2, 0)
        if slot == slots - 1:
            back(i + 1, 3)
            front(i + 2, 1)

    def project(j, t, b):
        at = pl.ds(t * tile, tile)
        return jnp.dot(
            mod[b * rows : (b + 1) * rows, :], wfull[j, :, at], preferred_element_type=F32
        )

    def finish(j, t, b, y):
        if j == 2:
            y = y.astype(BF16)
            for hh in range(per_tile):
                vbuf[b * heads + t * per_tile + hh] = y[:, hh * HEAD_DIM : (hh + 1) * HEAD_DIM]
            return
        swapped = jnp.dot(y.astype(BF16), mix[0, :tile, :tile], preferred_element_type=F32)
        square = jnp.dot((y * y).astype(BF16), mix[1, :tile, :tile], preferred_element_type=F32)
        inverse = lax.rsqrt(square + 1e-06)
        dest = kbuf if j == 1 else qbuf
        for hh in range(per_tile):
            at = slice(hh * HEAD_DIM, (hh + 1) * HEAD_DIM)
            turned = y[:, at] * tab[2 * j] + swapped[:, at] * tab[2 * j + 1]
            dest[b * heads + t * per_tile + hh] = (turned * inverse[:, at]).astype(BF16)

    def attend(span, first):
        ahead = {}
        for n in range(len(span) + 2):
            if n < len(span):
                h = span[n]
                ahead[n] = lax.dot_general(
                    qbuf[h], kbuf[h], (((1,), (1,)), ((), ())), preferred_element_type=F32
                )
            if n < 2:
                continue
            h = span[n - 2]
            expo = jnp.exp2(ahead.pop(n - 2))
            folded = expo[:, :HEAD_DIM]
            for k in range(1, rows // HEAD_DIM):
                folded = folded + expo[:, k * HEAD_DIM : (k + 1) * HEAD_DIM]
            mixed = jnp.dot(expo.astype(BF16), vbuf[h], preferred_element_type=F32)
            if first:
                lsum[h] = folded
                acc[h] = mixed
            else:
                lsum[h] += folded
                acc[h] += mixed

    def tables(o, first):
        place = lax.dot_general(
            pos[o], pick[...], (((0,), (0,)), ((), ())), preferred_element_type=F32
        )
        turns = place * rot[0:1, :]
        angle = (turns - jnp.floor(turns + 0.5)) * math.pi
        square = angle * angle
        low = angle * horner(SIN, square)
        cosine = 1.0 - 2.0 * low * low
        sine = 2.0 * low * horner(COS, square)
        for j in range(0 if first else 1, 2):
            strength = scale if j == 0 else 1.0
            tab[2 * j] = cosine * (gain_rows[j][0:1] * strength)
            tab[2 * j + 1] = sine * (gain_rows[j][1:2] * strength)

    swap_abs = jnp.abs(mix[0, :HEAD_DIM, :HEAD_DIM].astype(F32))
    gain_rows = []
    for j in range(2):
        own = gains[j : j + 1, :]
        column = jnp.sum(
            jnp.where(
                lax.broadcasted_iota(jnp.int32, (HEAD_DIM, HEAD_DIM), 0)
                == lax.broadcasted_iota(jnp.int32, (HEAD_DIM, HEAD_DIM), 1),
                own,
                0.0,
            ),
            axis=1,
            keepdims=True,
        )
        gain_rows.append(jnp.concatenate([own, jnp.sum(swap_abs * column, axis=0, keepdims=True)]))

    def modulate(o, core):
        @pl.loop(0, half_rows // STRIP, unroll=U_MOD)
        def _(r):
            start = aligned(core * (half_rows // STRIP) + r, STRIP)
            normed = lat[o, pl.ds(start, STRIP), :].astype(F32)
            for b in range(2):
                mod[pl.ds(pl.multiple_of(b * rows + start, STRIP), STRIP), :] = (
                    normed * (1.0 + modulation[1, b : b + 1, :]) + modulation[0, b : b + 1, :]
                ).astype(BF16)

    def step(i, first):
        o = order(i)
        tables(o, first)
        modulate(o, c)
        if not first:
            for s in range(subs):
                copy_c(o, s, other).wait_recv()
        modulate(o, other)

        pending = None
        for j in range(0 if first else 1, 3):
            if first:
                w_local[j].wait()
                w_copy[j].wait_recv()
            for t in range(tiles):
                for b in range(2):
                    y = project(j, t, b)
                    if pending is not None:
                        finish(*pending)
                    pending = (j, t, b, y)
                if j > 0:
                    pump(i, (j - 1) * tiles + t)
                    continue
                if t == max(tiles - 2, 0):
                    front(1, 0)
                if t == tiles - 1:
                    front(1, 1)
        finish(*pending)
        group = heads
        for g in range(2):
            attend(list(range(g * group, (g + 1) * group)), first)
            pump(i, 2 * tiles + g)

    step(0, True)

    @pl.loop(1, seq_n)
    def _(i):
        step(i, False)

    txt_local.wait()
    len_local.wait()
    copy_l(other).wait_recv()

    @pl.loop(0, seq_n)
    def _(o):
        copy_u(o).wait_recv()

    text_rows = txt.shape[2]
    count = seq_n * text_rows

    def copy_o(core, branch):
        at = pl.ds(aligned(branch, out_rows), out_rows)
        return remote(
            attf.at[core, :, at], attf.at[core, :, at], send_o.at[branch], recv_o.at[branch], cfg=other
        )

    for own in range(2):
        branch = c if own == 0 else other
        source = txt if own == 0 else txo
        base = aligned(c, mine) if own == 0 else 0
        valid = lax.broadcasted_iota(jnp.int32, (1, count), 1).astype(F32) < lens[branch, 0:1, :]
        ahead = {}
        for step_n in range(heads + 2):
            if step_n < heads:
                src = pl.ds(pl.multiple_of(base + step_n * HEAD_DIM, HEAD_DIM), HEAD_DIM)
                raw = source[:, 0, :, src].reshape(count, HEAD_DIM).astype(F32)
                inverse = lax.rsqrt(jnp.mean(raw * raw, axis=-1, keepdims=True) + 1e-06)
                keys = (raw * inverse * gains[1:2, :]).astype(BF16)
                ahead[step_n] = lax.dot_general(
                    qbuf[branch * heads + step_n], keys, (((1,), (1,)), ((), ())), preferred_element_type=F32
                )
            if step_n < 2:
                continue
            h = step_n - 2
            n = branch * heads + h
            src = pl.ds(pl.multiple_of(base + h * HEAD_DIM, HEAD_DIM), HEAD_DIM)
            values = source[:, 1, :, src].reshape(count, HEAD_DIM)
            expo = jnp.where(valid, jnp.exp2(ahead.pop(h)), 0.0)
            total = jnp.sum(lsum[n], axis=-1, keepdims=True) + jnp.sum(
                expo, axis=-1, keepdims=True
            )
            mixed = acc[n] + jnp.dot(expo.astype(BF16), values, preferred_element_type=F32)
            result = (mixed * (1.0 / total)).astype(BF16)
            for t in range(ten_n):
                attf[c, t, pl.ds(aligned(branch, out_rows), out_rows), h * HEAD_DIM : (h + 1) * HEAD_DIM] = (
                    result[t * out_rows : (t + 1) * out_rows]
                )

        copy_o(c, branch).start()

    out_local.wait()
    copy_o(other, other).wait_recv()
    copy_o(other, c).wait_recv()

    out_tile = 256 if out_cols % 256 == 0 else 128
    out_tiles = out_cols // out_tile

    def copy_r(t, k):
        return remote(
            part.at[t, k], got.at[t, k], send_r.at[t, k], recv_r.at[t, k], tensor=(x + t) % ten_n
        )

    strength = guide[0:1, 0:1]

    def out_block(t, k):
        to = (x + t) % ten_n
        at = pl.ds(k * out_tile, out_tile)
        y = jnp.dot(attf[0, to], wout[0:mine, at], preferred_element_type=F32)
        y = y + jnp.dot(attf[1, to], wout[mine : 2 * mine, at], preferred_element_type=F32)
        at_gate = pl.ds(pl.multiple_of(c * out_cols + k * out_tile, out_tile), out_tile)
        return (
            y[:out_rows] * (strength * modulation[2, 0:1, at_gate])
            + y[out_rows:] * ((1.0 - strength) * modulation[2, 1:2, at_gate])
        )

    for t in range(1, ten_n):
        for k in range(out_tiles):
            part[t, k] = out_block(t, k).astype(BF16)
            copy_r(t, k).start()

    for k in range(out_tiles):
        part[0, k] = out_block(0, k).astype(BF16)

    for k in range(out_tiles):
        total = part[0, k].astype(F32)
        for t in range(1, ten_n):
            copy_r(t, k).wait_recv()
            total = total + got[t, k].astype(F32)
        out[:, k * out_tile : (k + 1) * out_tile] = total.astype(BF16)

    for j in range(3):
        w_copy[j].wait_send()
    copy_l(c).wait_send()
    for b in range(2):
        copy_o(c, b).wait_send()
    for t in range(1, ten_n):
        for k in range(out_tiles):
            copy_r(t, k).wait_send()

    @pl.loop(0, seq_n)
    def _(o):
        copy_u(o).wait_send()

        @pl.when(o != z)
        def _():
            for s in range(subs):
                for t in range(1, ten_n):
                    copy_b(o, s, t).wait_send()
                copy_c(o, s, c).wait_send()

        for d in (1, -1):
            ahead = jnp.logical_or(o == z, d * (z - o) > 0)

            @pl.when(jnp.logical_and(ahead, inside(z + d)))
            def _():
                copy_p(o, d).wait_send()
                copy_t(o, d).wait_send()
                for s in range(subs):
                    copy_a(o, s, d).wait_send()


def local(
    seq_n, ten_n, latent, positions, text_kv, text_len, modulation, w_qkv, norm_gains, w_out, guidance
):
    rows, width = latent.shape
    mine = w_qkv.shape[2] // 2
    heads = mine // HEAD_DIM
    text_dev = text_kv.shape[2]
    out_rows = rows // ten_n
    out_cols = w_out.shape[1]
    out_tile = 256 if out_cols % 256 == 0 else 128
    out_tiles = out_cols // out_tile
    subs = rows // (2 * ten_n * STRIP)
    pos_in = jnp.pad(positions.astype(BF16), ((0, 13), (0, 0)))
    lens = jnp.broadcast_to(text_len.astype(F32)[None, :], (8, seq_n * text_dev))
    any_space = pl.BlockSpec(memory_space=pl.ANY)
    vmem = pl.BlockSpec(memory_space=pltpu.VMEM)
    dma = pltpu.SemaphoreType.DMA
    return pl.pallas_call(
        functools.partial(kernel, seq_n, ten_n),
        out_shape=jax.ShapeDtypeStruct((out_rows, out_cols), BF16),
        in_specs=[
            any_space,
            any_space,
            any_space,
            any_space,
            vmem,
            any_space,
            vmem,
            any_space,
            vmem,
            vmem,
            vmem,
            vmem,
        ],
        out_specs=vmem,
        scratch_shapes=[
            pltpu.VMEM((seq_n, rows, width), BF16),
            pltpu.VMEM((seq_n, 16, rows), BF16),
            pltpu.VMEM((seq_n, 2, text_dev, 2 * mine), BF16),
            pltpu.VMEM((seq_n, 2, text_dev, mine), BF16),
            pltpu.VMEM((2, 8, seq_n * text_dev), F32),
            pltpu.VMEM((3, width, mine), BF16),
            pltpu.VMEM(w_out.shape, BF16),
            pltpu.VMEM((2 * rows, width), BF16),
            pltpu.VMEM((4, rows, HEAD_DIM), F32),
            pltpu.VMEM((2 * heads, rows, HEAD_DIM), BF16),
            pltpu.VMEM((2 * heads, rows, HEAD_DIM), BF16),
            pltpu.VMEM((2 * heads, rows, HEAD_DIM), BF16),
            pltpu.VMEM((2 * heads, rows, HEAD_DIM), F32),
            pltpu.VMEM((2 * heads, rows, HEAD_DIM), F32),
            pltpu.VMEM((2, ten_n, 2 * out_rows, mine), BF16),
            pltpu.VMEM((ten_n, out_tiles, out_rows, out_tile), BF16),
            pltpu.VMEM((ten_n, out_tiles, out_rows, out_tile), BF16),
            dma((seq_n, subs, 2)),
            dma((seq_n, subs)),
            dma((seq_n, subs, ten_n)),
            dma((seq_n, subs, ten_n)),
            dma((seq_n, subs)),
            dma((seq_n, subs)),
            dma((seq_n, 2)),
            dma((seq_n,)),
            dma((seq_n, 2)),
            dma((seq_n,)),
            dma((seq_n,)),
            dma((seq_n,)),
            dma((3,)),
            dma((3,)),
            dma((1,)),
            dma((1,)),
            dma((2,)),
            dma((2,)),
            dma((ten_n, out_tiles)),
            dma((ten_n, out_tiles)),
            dma((8,)),
        ],
        compiler_params=pltpu.CompilerParams(
            collective_id=0, has_side_effects=True, vmem_limit_bytes=64 * 1024 * 1024 - 65536
        ),
    )(
        latent,
        pos_in,
        text_kv,
        lens,
        modulation,
        w_qkv,
        norm_gains,
        w_out,
        guidance.reshape(1, 1),
        jnp.asarray(ROT_ROWS),
        jnp.asarray(ROT_PICK, BF16),
        jnp.asarray(MIX, BF16),
    )


def solution(mesh):
    placed = (
        P(("groups", "seq"), None),
        P(None, ("groups", "seq")),
        P("cfg", None, ("groups", "seq"), "tensor"),
        P(("groups", "cfg")),
        P(None, "groups", None),
        P(None, "cfg", "tensor"),
        P(),
        P("tensor", "cfg"),
        P("groups"),
    )
    return jax.shard_map(
        functools.partial(local, mesh.shape["seq"], mesh.shape["tensor"]),
        mesh=mesh,
        in_specs=placed,
        out_specs=P(("groups", "seq", "tensor"), "cfg"),
        check_vma=False,
    )
```

```python
import functools
import math

import jax
import jax.numpy as jnp
import numpy as np
from jax import lax
from jax.experimental import pallas as pl
from jax.experimental.pallas import tpu as pltpu
from jax.sharding import PartitionSpec as P

HEAD_DIM = 128
MESH = pl.DeviceIdType.MESH
U_MOD = 8
F32 = jnp.float32
BF16 = jnp.bfloat16


def rotary_rows(head_size):
    rows = np.zeros((8, head_size), np.float32)
    swap = np.zeros((head_size, head_size), np.float32)
    axes = np.zeros((head_size,), np.int32)
    blocks = (head_size // 8, 7 * head_size // 16, 7 * head_size // 16)
    offset = 0
    for axis_id, width in enumerate(blocks):
        half = width // 2
        turns = 256.0 ** (-np.arange(half, dtype=np.float64) / half) / (2 * np.pi)
        rows[0, offset : offset + half] = turns
        rows[0, offset + half : offset + width] = turns
        for k in range(half):
            swap[offset + half + k, offset + k] = -1.0
            swap[offset + k, offset + half + k] = 1.0
        axes[offset : offset + width] = axis_id
        offset += width
    return rows, axes, swap


ROT_ROWS, ROT_AXES, ROT_SWAP = rotary_rows(HEAD_DIM)
ROT_PICK = (np.arange(16)[:, None] == ROT_AXES[None, :]).astype(np.float32)
SIDE = np.kron(np.eye(2), np.ones((HEAD_DIM, HEAD_DIM)))
MIX = np.stack([np.kron(np.eye(2), ROT_SWAP), SIDE / HEAD_DIM]).astype(np.float32)
SIN = tuple((-1.0) ** k / math.factorial(2 * k + 1) for k in range(6))
COS = tuple((-1.0) ** k / math.factorial(2 * k) for k in range(6))
LOG2E = 1.4426950408889634


def horner(terms, value):
    total = terms[-1]
    for term in terms[-2::-1]:
        total = total * value + term
    return total


STRIP = 16


def kernel(
    seq_n,
    ten_n,
    latent,
    pos_in,
    text_kv,
    lens_in,
    modulation,
    w_qkv,
    gains,
    w_out,
    guide,
    rot,
    pick,
    mix,
    out,
    lat,
    pos,
    txt,
    txo,
    lens,
    wfull,
    wout,
    mod,
    tab,
    qbuf,
    kbuf,
    vbuf,
    acc,
    lsum,
    attf,
    part,
    got,
    send_a,
    recv_a,
    send_b,
    recv_b,
    send_c,
    recv_c,
    send_p,
    recv_p,
    send_t,
    recv_t,
    send_u,
    recv_u,
    send_w,
    recv_w,
    send_l,
    recv_l,
    send_o,
    recv_o,
    send_r,
    recv_r,
    loc,
):
    x = lax.axis_index("tensor")
    c = lax.axis_index("cfg")
    z = lax.axis_index("seq")
    other = 1 - c
    rows, width = latent.shape
    half = w_qkv.shape[1]
    mine = wfull.shape[2]
    heads = mine // HEAD_DIM
    half_rows = rows // 2
    band = ten_n * STRIP
    subs = half_rows // band
    out_rows = rows // ten_n
    out_cols = w_out.shape[1]
    scale = HEAD_DIM ** (-0.5) * LOG2E
    tile = 256 if mine % 256 == 0 else 128
    per_tile = tile // HEAD_DIM
    tiles = mine // tile
    shorter = jnp.minimum(z, seq_n - 1 - z)
    long_sign = jnp.where(2 * z < seq_n - 1, 1, -1)

    def order(i):
        near = i <= 2 * shorter
        dist = jnp.where(near, (i + 1) // 2, i - shorter)
        sign = jnp.where(near, 2 * (i % 2) - 1, long_sign)
        return jnp.where(i == 0, z, z + dist * sign)

    def remote(src, dst, send, recv, **to):
        return pltpu.make_async_remote_copy(
            src_ref=src, dst_ref=dst, send_sem=send, recv_sem=recv, device_id=to, device_id_type=MESH
        )

    def aligned(value, unit):
        return pl.multiple_of(value * unit, unit)

    def inside(o):
        return jnp.logical_and(o >= 0, o < seq_n)

    cols_of = lambda core: pl.ds(aligned(core, mine), mine)
    w_copy = [
        remote(
            w_qkv.at[j, :, cols_of(other)],
            wfull.at[j, pl.ds(aligned(c, half), half), :],
            send_w.at[j],
            recv_w.at[j],
            cfg=other,
        )
        for j in range(3)
    ]
    w_local = [
        pltpu.make_async_copy(
            w_qkv.at[j, :, cols_of(c)], wfull.at[j, pl.ds(aligned(c, half), half), :], loc.at[j]
        )
        for j in range(3)
    ]
    lat_local = pltpu.make_async_copy(latent, lat.at[z], loc.at[3])
    pos_local = pltpu.make_async_copy(pos_in, pos.at[z], loc.at[4])
    txt_local = pltpu.make_async_copy(text_kv.at[0], txt.at[z], loc.at[5])
    len_local = pltpu.make_async_copy(lens_in, lens.at[c], loc.at[6])
    out_local = pltpu.make_async_copy(w_out, wout, loc.at[7])

    def strip_of(core, s, ten):
        return pl.ds(aligned((core * subs + s) * ten_n + ten, STRIP), STRIP)

    def band_of(core, s):
        return pl.ds(aligned(core * subs + s, band), band)

    def up(d):
        return 0 if d > 0 else 1

    def copy_a(o, s, d):
        at = strip_of(c, s, x)
        return remote(lat.at[o, at], lat.at[o, at], send_a.at[o, s, up(d)], recv_a.at[o, s], seq=z + d)

    def copy_b(o, s, t):
        at = strip_of(c, s, x)
        to = (x + t) % ten_n
        return remote(lat.at[o, at], lat.at[o, at], send_b.at[o, s, t], recv_b.at[o, s, t], tensor=to)

    def arrived_b(o, s, t):
        source = (x + ten_n - t) % ten_n
        at = strip_of(c, s, source)
        return remote(lat.at[o, at], lat.at[o, at], send_b.at[o, s, t], recv_b.at[o, s, t], tensor=source)

    def copy_c(o, s, core):
        at = band_of(core, s)
        return remote(lat.at[o, at], lat.at[o, at], send_c.at[o, s], recv_c.at[o, s], cfg=other)

    def first_p(d):
        return remote(pos_in, pos.at[z], send_p.at[z, up(d)], recv_p.at[z], seq=z + d)

    def copy_p(o, d):
        return remote(pos.at[o], pos.at[o], send_p.at[o, up(d)], recv_p.at[o], seq=z + d)

    def first_t(d):
        return remote(text_kv.at[0], txt.at[z], send_t.at[z, up(d)], recv_t.at[z], seq=z + d)

    def copy_t(o, d):
        return remote(txt.at[o], txt.at[o], send_t.at[o, up(d)], recv_t.at[o], seq=z + d)

    def first_u():
        return remote(
            text_kv.at[0, :, :, cols_of(other)], txo.at[z], send_u.at[z], recv_u.at[z], cfg=other
        )

    def copy_u(o):
        return remote(txt.at[o, :, :, cols_of(other)], txo.at[o], send_u.at[o], recv_u.at[o], cfg=other)

    def copy_l(core):
        return remote(lens_in, lens.at[core], send_l.at[0], recv_l.at[0], cfg=other)

    for j in range(3):
        w_local[j].start()
    lat_local.start()
    pos_local.start()
    txt_local.start()
    len_local.start()
    out_local.start()

    barrier = pltpu.get_barrier_semaphore()
    for d in (1, -1):

        @pl.when(inside(z + d))
        def _():
            pl.semaphore_signal(barrier, inc=1, device_id={"seq": z + d}, device_id_type=MESH)

    pl.semaphore_signal(barrier, inc=1, device_id={"cfg": other}, device_id_type=MESH)
    for t in range(1, ten_n):
        pl.semaphore_signal(
            barrier, inc=1, device_id={"tensor": (x + t) % ten_n}, device_id_type=MESH
        )

    def normalize(at):
        value = lat[z, at, :].astype(F32)
        center = value - jnp.mean(value, axis=-1, keepdims=True)
        normed = center * lax.rsqrt(jnp.mean(center * center, axis=-1, keepdims=True) + 1e-06)
        lat[z, at, :] = normed.astype(BF16)

    lat_local.wait()
    for s in range(subs):
        normalize(strip_of(c, s, x))

    sides = jnp.where(z > 0, 1, 0) + jnp.where(z < seq_n - 1, 1, 0)
    pl.semaphore_wait(barrier, ten_n + sides)

    for d in (1, -1):

        @pl.when(inside(z + d))
        def _():
            first_p(d).start()
            for s in range(subs):
                copy_a(z, s, d).start()

    for j in range(3):
        w_copy[j].start()
    copy_l(c).start()
    first_u().start()

    for t in range(1, ten_n):
        for s in range(subs):
            normalize(strip_of(c, s, (x + t) % ten_n))

    @pl.loop(0, half_rows // STRIP, unroll=4)
    def _(r):
        normalize(pl.ds(aligned(other * (half_rows // STRIP) + r, STRIP), STRIP))

    pos_local.wait()

    def pump_a(k, s):
        for d in (1, -1):
            o = z - d * k

            @pl.when(inside(o))
            def _():
                if s == 0:
                    copy_p(o, d).wait_recv()
                copy_a(o, s, d).wait_recv()

                @pl.when(inside(z + d))
                def _():
                    if s == 0:
                        copy_p(o, d).start()
                    copy_a(o, s, d).start()

    def pump_t(k):
        for d in (1, -1):
            o = z - d * k

            @pl.when(inside(o))
            def _():
                copy_t(o, d).wait_recv()

                @pl.when(inside(z + d))
                def _():
                    copy_t(o, d).start()

                copy_u(o).start()

    def start_b(o, s):
        for t in range(1, ten_n):
            copy_b(o, s, t).start()

    def end_b(o, s):
        for t in range(1, ten_n):
            arrived_b(o, s, t).wait_recv()
        copy_c(o, s, c).start()

    def front(k, p):
        @pl.when(k < seq_n)
        def _():
            for s in range(subs):
                if s * 4 // subs == p:
                    pump_a(k, s)
                    start_b(order(k), s)

    def back(k, p):
        @pl.when(k < seq_n)
        def _():
            for s in range(subs):
                if s * 4 // subs == p:
                    end_b(order(k), s)

    slots = 2 * tiles + 2

    def text_front(i, slot):
        last = seq_n - 1
        if slot == tiles:
            for d in (1, -1):

                @pl.when(jnp.logical_and(i == 1, inside(z + d)))
                def _():
                    first_t(d).start()

        if slot == 1 and last > 1:

            @pl.when(i == last)
            def _():
                pump_t(last - 1)

        if slot == 2 * tiles - 1:

            @pl.when(jnp.logical_or(jnp.logical_and(i > 1, i < last), i == last))
            def _():
                pump_t(jnp.where(i == last, last, i - 1))

    def pump(i, slot):
        if slot == 0:
            front(i + 1, 2)
        if slot == min(2, 2 * tiles - 1):
            front(i + 1, 3)
        if slot == tiles:
            back(i + 1, 0)
        if slot == 2 * tiles - 1:
            back(i + 1, 1)
        if slot == 2 * tiles:
            back(i + 1, 2)
            front(i + 2, 0)
        if slot == slots - 1:
            back(i + 1, 3)
            front(i + 2, 1)
        text_front(i, slot)

    def project(j, t, b):
        at = pl.ds(t * tile, tile)
        return jnp.dot(
            mod[b * rows : (b + 1) * rows, :], wfull[j, :, at], preferred_element_type=F32
        )

    def finish(j, t, b, y):
        if j == 2:
            y = y.astype(BF16)
            for hh in range(per_tile):
                vbuf[b * heads + t * per_tile + hh] = y[:, hh * HEAD_DIM : (hh + 1) * HEAD_DIM]
            return
        swapped = jnp.dot(y.astype(BF16), mix[0, :tile, :tile], preferred_element_type=F32)
        square = jnp.dot((y * y).astype(BF16), mix[1, :tile, :tile], preferred_element_type=F32)
        inverse = lax.rsqrt(square + 1e-06)
        dest = kbuf if j == 1 else qbuf
        for hh in range(per_tile):
            at = slice(hh * HEAD_DIM, (hh + 1) * HEAD_DIM)
            turned = y[:, at] * tab[2 * j] + swapped[:, at] * tab[2 * j + 1]
            dest[b * heads + t * per_tile + hh] = (turned * inverse[:, at]).astype(BF16)

    def attend(span, first):
        ahead = {}
        for n in range(len(span) + 2):
            if n < len(span):
                h = span[n]
                ahead[n] = lax.dot_general(
                    qbuf[h], kbuf[h], (((1,), (1,)), ((), ())), preferred_element_type=F32
                )
            if n < 2:
                continue
            h = span[n - 2]
            expo = jnp.exp2(ahead.pop(n - 2))
            folded = expo[:, :HEAD_DIM]
            for k in range(1, rows // HEAD_DIM):
                folded = folded + expo[:, k * HEAD_DIM : (k + 1) * HEAD_DIM]
            mixed = jnp.dot(expo.astype(BF16), vbuf[h], preferred_element_type=F32)
            if first:
                lsum[h] = folded
                acc[h] = mixed
            else:
                lsum[h] += folded
                acc[h] += mixed

    def tables(o, first):
        place = lax.dot_general(
            pos[o], pick[...], (((0,), (0,)), ((), ())), preferred_element_type=F32
        )
        turns = place * rot[0:1, :]
        angle = (turns - jnp.floor(turns + 0.5)) * math.pi
        square = angle * angle
        low = angle * horner(SIN, square)
        cosine = 1.0 - 2.0 * low * low
        sine = 2.0 * low * horner(COS, square)
        for j in range(0 if first else 1, 2):
            strength = scale if j == 0 else 1.0
            tab[2 * j] = cosine * (gain_rows[j][0:1] * strength)
            tab[2 * j + 1] = sine * (gain_rows[j][1:2] * strength)

    swap_abs = jnp.abs(mix[0, :HEAD_DIM, :HEAD_DIM].astype(F32))
    gain_rows = []
    for j in range(2):
        own = gains[j : j + 1, :]
        column = jnp.sum(
            jnp.where(
                lax.broadcasted_iota(jnp.int32, (HEAD_DIM, HEAD_DIM), 0)
                == lax.broadcasted_iota(jnp.int32, (HEAD_DIM, HEAD_DIM), 1),
                own,
                0.0,
            ),
            axis=1,
            keepdims=True,
        )
        gain_rows.append(jnp.concatenate([own, jnp.sum(swap_abs * column, axis=0, keepdims=True)]))

    def modulate(o, core):
        @pl.loop(0, half_rows // STRIP, unroll=U_MOD)
        def _(r):
            start = aligned(core * (half_rows // STRIP) + r, STRIP)
            normed = lat[o, pl.ds(start, STRIP), :].astype(F32)
            for b in range(2):
                mod[pl.ds(pl.multiple_of(b * rows + start, STRIP), STRIP), :] = (
                    normed * (1.0 + modulation[1, b : b + 1, :]) + modulation[0, b : b + 1, :]
                ).astype(BF16)

    def step(i, first):
        o = order(i)
        tables(o, first)
        modulate(o, c)
        if not first:
            for s in range(subs):
                copy_c(o, s, other).wait_recv()
        modulate(o, other)

        pending = None
        for j in range(0 if first else 1, 3):
            if first:
                w_local[j].wait()
                w_copy[j].wait_recv()
            for t in range(tiles):
                for b in range(2):
                    y = project(j, t, b)
                    if pending is not None:
                        finish(*pending)
                    pending = (j, t, b, y)
                if j > 0:
                    pump(i, (j - 1) * tiles + t)
                    continue
                if t == max(tiles - 2, 0):
                    front(1, 0)
                if t == tiles - 1:
                    front(1, 1)
        finish(*pending)
        group = heads
        for g in range(2):
            attend(list(range(g * group, (g + 1) * group)), first)
            pump(i, 2 * tiles + g)

    step(0, True)

    @pl.loop(1, seq_n)
    def _(i):
        step(i, False)

    txt_local.wait()
    len_local.wait()
    copy_l(other).wait_recv()

    @pl.loop(0, seq_n)
    def _(o):
        copy_u(o).wait_recv()

    text_rows = txt.shape[2]
    count = seq_n * text_rows

    def copy_o(core, t, own):
        to = (x + t) % ten_n
        branch = core if own == 0 else 1 - core
        at = pl.ds(aligned(branch, out_rows), out_rows)
        place = attf.at[core, to, at]
        return remote(place, place, send_o.at[t, own], recv_o.at[t, own], cfg=other)

    def text(t, own):
        to = (x + t) % ten_n
        here = pl.ds(aligned(to, out_rows), out_rows)
        branch = c if own == 0 else other
        source = txt if own == 0 else txo
        base = aligned(c, mine) if own == 0 else 0
        valid = lax.broadcasted_iota(jnp.int32, (1, count), 1).astype(F32) < lens[branch, 0:1, :]
        ahead = {}
        for n in range(heads + 2):
            if n < heads:
                src = pl.ds(pl.multiple_of(base + n * HEAD_DIM, HEAD_DIM), HEAD_DIM)
                raw = source[:, 0, :, src].reshape(count, HEAD_DIM).astype(F32)
                inverse = lax.rsqrt(jnp.mean(raw * raw, axis=-1, keepdims=True) + 1e-06)
                keys = (raw * inverse * gains[1:2, :]).astype(BF16)
                ahead[n] = lax.dot_general(
                    qbuf[branch * heads + n, here, :],
                    keys,
                    (((1,), (1,)), ((), ())),
                    preferred_element_type=F32,
                )
            if n < 2:
                continue
            h = n - 2
            row = branch * heads + h
            src = pl.ds(pl.multiple_of(base + h * HEAD_DIM, HEAD_DIM), HEAD_DIM)
            values = source[:, 1, :, src].reshape(count, HEAD_DIM)
            expo = jnp.where(valid, jnp.exp2(ahead.pop(h)), 0.0)
            total = jnp.sum(lsum[row, here, :], axis=-1, keepdims=True) + jnp.sum(
                expo, axis=-1, keepdims=True
            )
            mixed = acc[row, here, :] + jnp.dot(
                expo.astype(BF16), values, preferred_element_type=F32
            )
            attf[
                c, to, pl.ds(aligned(branch, out_rows), out_rows), h * HEAD_DIM : (h + 1) * HEAD_DIM
            ] = (mixed * (1.0 / total)).astype(BF16)
        copy_o(c, t, own).start()

    out_tile = 256 if out_cols % 256 == 0 else 128
    out_tiles = out_cols // out_tile

    def copy_r(t, k):
        return remote(
            part.at[t, k], got.at[t, k], send_r.at[t, k], recv_r.at[t, k], tensor=(x + t) % ten_n
        )

    strength = guide[0:1, 0:1]

    def out_block(t, k):
        to = (x + t) % ten_n
        at = pl.ds(k * out_tile, out_tile)
        y = jnp.dot(attf[0, to], wout[0:mine, at], preferred_element_type=F32)
        y = y + jnp.dot(attf[1, to], wout[mine : 2 * mine, at], preferred_element_type=F32)
        at_gate = pl.ds(pl.multiple_of(c * out_cols + k * out_tile, out_tile), out_tile)
        return (
            y[:out_rows] * (strength * modulation[2, 0:1, at_gate])
            + y[out_rows:] * ((1.0 - strength) * modulation[2, 1:2, at_gate])
        )

    turn = list(range(1, ten_n)) + [0]
    text(turn[0], 0)
    text(turn[0], 1)
    out_local.wait()
    for n, t in enumerate(turn):
        if n + 1 < ten_n:
            text(turn[n + 1], 0)
        copy_o(other, t, 0).wait_recv()
        copy_o(other, t, 1).wait_recv()
        for k in range(out_tiles):
            part[t, k] = out_block(t, k).astype(BF16)
            if t > 0:
                copy_r(t, k).start()
        if n + 1 < ten_n:
            text(turn[n + 1], 1)

    for k in range(out_tiles):
        total = part[0, k].astype(F32)
        for t in range(1, ten_n):
            copy_r(t, k).wait_recv()
            total = total + got[t, k].astype(F32)
        out[:, k * out_tile : (k + 1) * out_tile] = total.astype(BF16)

    for j in range(3):
        w_copy[j].wait_send()
    copy_l(c).wait_send()
    for t in range(ten_n):
        for own in range(2):
            copy_o(c, t, own).wait_send()
    for t in range(1, ten_n):
        for k in range(out_tiles):
            copy_r(t, k).wait_send()

    @pl.loop(0, seq_n)
    def _(o):
        copy_u(o).wait_send()

        @pl.when(o != z)
        def _():
            for s in range(subs):
                for t in range(1, ten_n):
                    copy_b(o, s, t).wait_send()
                copy_c(o, s, c).wait_send()

        for d in (1, -1):
            ahead = jnp.logical_or(o == z, d * (z - o) > 0)

            @pl.when(jnp.logical_and(ahead, inside(z + d)))
            def _():
                copy_p(o, d).wait_send()
                copy_t(o, d).wait_send()
                for s in range(subs):
                    copy_a(o, s, d).wait_send()


def local(
    seq_n, ten_n, latent, positions, text_kv, text_len, modulation, w_qkv, norm_gains, w_out, guidance
):
    rows, width = latent.shape
    mine = w_qkv.shape[2] // 2
    heads = mine // HEAD_DIM
    text_dev = text_kv.shape[2]
    out_rows = rows // ten_n
    out_cols = w_out.shape[1]
    out_tile = 256 if out_cols % 256 == 0 else 128
    out_tiles = out_cols // out_tile
    subs = rows // (2 * ten_n * STRIP)
    pos_in = jnp.pad(positions.astype(BF16), ((0, 13), (0, 0)))
    lens = jnp.broadcast_to(text_len.astype(F32)[None, :], (8, seq_n * text_dev))
    any_space = pl.BlockSpec(memory_space=pl.ANY)
    vmem = pl.BlockSpec(memory_space=pltpu.VMEM)
    dma = pltpu.SemaphoreType.DMA
    return pl.pallas_call(
        functools.partial(kernel, seq_n, ten_n),
        out_shape=jax.ShapeDtypeStruct((out_rows, out_cols), BF16),
        in_specs=[
            any_space,
            any_space,
            any_space,
            any_space,
            vmem,
            any_space,
            vmem,
            any_space,
            vmem,
            vmem,
            vmem,
            vmem,
        ],
        out_specs=vmem,
        scratch_shapes=[
            pltpu.VMEM((seq_n, rows, width), BF16),
            pltpu.VMEM((seq_n, 16, rows), BF16),
            pltpu.VMEM((seq_n, 2, text_dev, 2 * mine), BF16),
            pltpu.VMEM((seq_n, 2, text_dev, mine), BF16),
            pltpu.VMEM((2, 8, seq_n * text_dev), F32),
            pltpu.VMEM((3, width, mine), BF16),
            pltpu.VMEM(w_out.shape, BF16),
            pltpu.VMEM((2 * rows, width), BF16),
            pltpu.VMEM((4, rows, HEAD_DIM), F32),
            pltpu.VMEM((2 * heads, rows, HEAD_DIM), BF16),
            pltpu.VMEM((2 * heads, rows, HEAD_DIM), BF16),
            pltpu.VMEM((2 * heads, rows, HEAD_DIM), BF16),
            pltpu.VMEM((2 * heads, rows, HEAD_DIM), F32),
            pltpu.VMEM((2 * heads, rows, HEAD_DIM), F32),
            pltpu.VMEM((2, ten_n, 2 * out_rows, mine), BF16),
            pltpu.VMEM((ten_n, out_tiles, out_rows, out_tile), BF16),
            pltpu.VMEM((ten_n, out_tiles, out_rows, out_tile), BF16),
            dma((seq_n, subs, 2)),
            dma((seq_n, subs)),
            dma((seq_n, subs, ten_n)),
            dma((seq_n, subs, ten_n)),
            dma((seq_n, subs)),
            dma((seq_n, subs)),
            dma((seq_n, 2)),
            dma((seq_n,)),
            dma((seq_n, 2)),
            dma((seq_n,)),
            dma((seq_n,)),
            dma((seq_n,)),
            dma((3,)),
            dma((3,)),
            dma((1,)),
            dma((1,)),
            dma((ten_n, 2)),
            dma((ten_n, 2)),
            dma((ten_n, out_tiles)),
            dma((ten_n, out_tiles)),
            dma((8,)),
        ],
        compiler_params=pltpu.CompilerParams(
            collective_id=0, has_side_effects=True, vmem_limit_bytes=64 * 1024 * 1024 - 65536
        ),
    )(
        latent,
        pos_in,
        text_kv,
        lens,
        modulation,
        w_qkv,
        norm_gains,
        w_out,
        guidance.reshape(1, 1),
        jnp.asarray(ROT_ROWS),
        jnp.asarray(ROT_PICK, BF16),
        jnp.asarray(MIX, BF16),
    )


def solution(mesh):
    placed = (
        P(("groups", "seq"), None),
        P(None, ("groups", "seq")),
        P("cfg", None, ("groups", "seq"), "tensor"),
        P(("groups", "cfg")),
        P(None, "groups", None),
        P(None, "cfg", "tensor"),
        P(),
        P("tensor", "cfg"),
        P("groups"),
    )
    return jax.shard_map(
        functools.partial(local, mesh.shape["seq"], mesh.shape["tensor"]),
        mesh=mesh,
        in_specs=placed,
        out_specs=P(("groups", "seq", "tensor"), "cfg"),
        check_vma=False,
    )
```

```python
import functools
import math

import jax
import jax.numpy as jnp
import numpy as np
from jax import lax
from jax.experimental import pallas as pl
from jax.experimental.pallas import tpu as pltpu
from jax.sharding import PartitionSpec as P

HEAD_DIM = 128
MESH = pl.DeviceIdType.MESH
U_MOD = 8
F32 = jnp.float32
BF16 = jnp.bfloat16


def rotary_rows(head_size):
    rows = np.zeros((8, head_size), np.float32)
    swap = np.zeros((head_size, head_size), np.float32)
    axes = np.zeros((head_size,), np.int32)
    blocks = (head_size // 8, 7 * head_size // 16, 7 * head_size // 16)
    offset = 0
    for axis_id, width in enumerate(blocks):
        half = width // 2
        turns = 256.0 ** (-np.arange(half, dtype=np.float64) / half) / (2 * np.pi)
        rows[0, offset : offset + half] = turns
        rows[0, offset + half : offset + width] = turns
        for k in range(half):
            swap[offset + half + k, offset + k] = -1.0
            swap[offset + k, offset + half + k] = 1.0
        axes[offset : offset + width] = axis_id
        offset += width
    return rows, axes, swap


ROT_ROWS, ROT_AXES, ROT_SWAP = rotary_rows(HEAD_DIM)
ROT_PICK = (np.arange(16)[:, None] == ROT_AXES[None, :]).astype(np.float32)
SIDE = np.kron(np.eye(2), np.ones((HEAD_DIM, HEAD_DIM)))
MIX = np.stack([np.kron(np.eye(2), ROT_SWAP), SIDE / HEAD_DIM]).astype(np.float32)
SIN = tuple((-1.0) ** k / math.factorial(2 * k + 1) for k in range(6))
COS = tuple((-1.0) ** k / math.factorial(2 * k) for k in range(6))
LOG2E = 1.4426950408889634


def horner(terms, value):
    total = terms[-1]
    for term in terms[-2::-1]:
        total = total * value + term
    return total


STRIP = 16


def kernel(
    seq_n,
    ten_n,
    latent,
    pos_in,
    text_kv,
    lens_in,
    modulation,
    w_qkv,
    gains,
    w_out,
    guide,
    rot,
    pick,
    mix,
    out,
    lat,
    pos,
    txt,
    txo,
    lens,
    wfull,
    wout,
    mod,
    tab,
    qbuf,
    kbuf,
    vbuf,
    acc,
    lsum,
    attf,
    part,
    got,
    send_a,
    recv_a,
    send_b,
    recv_b,
    send_c,
    recv_c,
    send_p,
    recv_p,
    send_t,
    recv_t,
    send_u,
    recv_u,
    send_w,
    recv_w,
    send_l,
    recv_l,
    send_o,
    recv_o,
    send_r,
    recv_r,
    loc,
):
    x = lax.axis_index("tensor")
    c = lax.axis_index("cfg")
    z = lax.axis_index("seq")
    other = 1 - c
    rows, width = latent.shape
    half = w_qkv.shape[1]
    mine = wfull.shape[2]
    heads = mine // HEAD_DIM
    half_rows = rows // 2
    band = ten_n * STRIP
    subs = half_rows // band
    out_rows = rows // ten_n
    out_cols = w_out.shape[1]
    scale = HEAD_DIM ** (-0.5) * LOG2E
    tile = 256 if mine % 256 == 0 else 128
    per_tile = tile // HEAD_DIM
    tiles = mine // tile
    shorter = jnp.minimum(z, seq_n - 1 - z)
    long_sign = jnp.where(2 * z < seq_n - 1, 1, -1)

    def order(i):
        near = i <= 2 * shorter
        dist = jnp.where(near, (i + 1) // 2, i - shorter)
        sign = jnp.where(near, 2 * (i % 2) - 1, long_sign)
        return jnp.where(i == 0, z, z + dist * sign)

    def remote(src, dst, send, recv, **to):
        return pltpu.make_async_remote_copy(
            src_ref=src, dst_ref=dst, send_sem=send, recv_sem=recv, device_id=to, device_id_type=MESH
        )

    def aligned(value, unit):
        return pl.multiple_of(value * unit, unit)

    def inside(o):
        return jnp.logical_and(o >= 0, o < seq_n)

    cols_of = lambda core: pl.ds(aligned(core, mine), mine)
    w_copy = [
        remote(
            w_qkv.at[j, :, cols_of(other)],
            wfull.at[j, pl.ds(aligned(c, half), half), :],
            send_w.at[j],
            recv_w.at[j],
            cfg=other,
        )
        for j in range(3)
    ]
    w_local = [
        pltpu.make_async_copy(
            w_qkv.at[j, :, cols_of(c)], wfull.at[j, pl.ds(aligned(c, half), half), :], loc.at[j]
        )
        for j in range(3)
    ]
    lat_local = pltpu.make_async_copy(latent, lat.at[z], loc.at[3])
    txt_local = pltpu.make_async_copy(text_kv.at[0], txt.at[z], loc.at[5])
    out_local = pltpu.make_async_copy(w_out, wout, loc.at[7])

    def strip_of(core, s, ten):
        return pl.ds(aligned((core * subs + s) * ten_n + ten, STRIP), STRIP)

    def band_of(core, s):
        return pl.ds(aligned(core * subs + s, band), band)

    def up(d):
        return 0 if d > 0 else 1

    def copy_a(o, s, d):
        at = strip_of(c, s, x)
        return remote(lat.at[o, at], lat.at[o, at], send_a.at[o, s, up(d)], recv_a.at[o, s], seq=z + d)

    def copy_b(o, s, t):
        at = strip_of(c, s, x)
        to = (x + t) % ten_n
        return remote(lat.at[o, at], lat.at[o, at], send_b.at[o, s, t], recv_b.at[o, s, t], tensor=to)

    def arrived_b(o, s, t):
        source = (x + ten_n - t) % ten_n
        at = strip_of(c, s, source)
        return remote(lat.at[o, at], lat.at[o, at], send_b.at[o, s, t], recv_b.at[o, s, t], tensor=source)

    def copy_c(o, s, core):
        at = band_of(core, s)
        return remote(lat.at[o, at], lat.at[o, at], send_c.at[o, s], recv_c.at[o, s], cfg=other)

    def first_p(d):
        return copy_p(z, d)

    def copy_p(o, d):
        return remote(pos.at[o], pos.at[o], send_p.at[o, up(d)], recv_p.at[o], seq=z + d)

    def first_t(d):
        return remote(text_kv.at[0], txt.at[z], send_t.at[z, up(d)], recv_t.at[z], seq=z + d)

    def copy_t(o, d):
        return remote(txt.at[o], txt.at[o], send_t.at[o, up(d)], recv_t.at[o], seq=z + d)

    def first_u():
        return remote(
            text_kv.at[0, :, :, cols_of(other)], txo.at[z], send_u.at[z], recv_u.at[z], cfg=other
        )

    def copy_u(o):
        return remote(txt.at[o, :, :, cols_of(other)], txo.at[o], send_u.at[o], recv_u.at[o], cfg=other)

    def copy_l(core):
        return remote(lens.at[core], lens.at[core], send_l.at[0], recv_l.at[0], cfg=other)

    lat_local.start()

    barrier = pltpu.get_barrier_semaphore()
    for d in (1, -1):

        @pl.when(inside(z + d))
        def _():
            pl.semaphore_signal(barrier, inc=1, device_id={"seq": z + d}, device_id_type=MESH)

    pl.semaphore_signal(barrier, inc=1, device_id={"cfg": other}, device_id_type=MESH)
    for t in range(1, ten_n):
        pl.semaphore_signal(
            barrier, inc=1, device_id={"tensor": (x + t) % ten_n}, device_id_type=MESH
        )

    def normalize(core, ten):
        spots = [strip_of(core, s, ten) for s in range(subs)]
        lanes = [slice(k * HEAD_DIM, (k + 1) * HEAD_DIM) for k in range(width // HEAD_DIM)]

        def mean_of(body):
            means = []
            for at in spots:
                total = body(at, lanes[0], len(means))
                for lane in lanes[1:]:
                    total = total + body(at, lane, len(means))
                means.append(jnp.sum(total, axis=-1, keepdims=True) * (1.0 / width))
            return means

        means = mean_of(lambda at, lane, n: lat[z, at, lane].astype(F32))

        def squared(at, lane, n):
            center = lat[z, at, lane].astype(F32) - means[n]
            return center * center

        inverses = [lax.rsqrt(power + 1e-06) for power in mean_of(squared)]
        for n, at in enumerate(spots):
            for lane in lanes:
                lat[z, at, lane] = (
                    (lat[z, at, lane].astype(F32) - means[n]) * inverses[n]
                ).astype(BF16)

    pos[z] = jnp.concatenate(
        [pos_in[...].astype(F32), jnp.zeros((16 - pos_in.shape[0], rows), F32)]
    ).astype(BF16)
    lens[c] = jnp.broadcast_to(lens_in[0:1, 0:1].astype(F32), lens.shape[1:])
    lat_local.wait()
    for j in range(3):
        w_local[j].start()
    txt_local.start()
    out_local.start()
    normalize(c, x)

    sides = jnp.where(z > 0, 1, 0) + jnp.where(z < seq_n - 1, 1, 0)
    pl.semaphore_wait(barrier, ten_n + sides)

    for d in (1, -1):

        @pl.when(inside(z + d))
        def _():
            first_p(d).start()
            for s in range(subs):
                copy_a(z, s, d).start()

    for j in range(3):
        w_copy[j].start()
    copy_l(c).start()
    first_u().start()

    @pl.loop(1, 2 * ten_n)
    def _(g):
        normalize(jnp.where(g < ten_n, c, other), (x + g) % ten_n)

    def pump_a(k, s):
        for d in (1, -1):
            o = z - d * k

            @pl.when(inside(o))
            def _():
                if s == 0:
                    copy_p(o, d).wait_recv()
                copy_a(o, s, d).wait_recv()

                @pl.when(inside(z + d))
                def _():
                    if s == 0:
                        copy_p(o, d).start()
                    copy_a(o, s, d).start()

    def pump_t(k):
        for d in (1, -1):
            o = z - d * k

            @pl.when(inside(o))
            def _():
                copy_t(o, d).wait_recv()

                @pl.when(inside(z + d))
                def _():
                    copy_t(o, d).start()

                copy_u(o).start()

    def start_b(o, s):
        for t in range(1, ten_n):
            copy_b(o, s, t).start()

    def end_b(o, s):
        for t in range(1, ten_n):
            arrived_b(o, s, t).wait_recv()
        copy_c(o, s, c).start()

    def front(k, p):
        @pl.when(k < seq_n)
        def _():
            for s in range(subs):
                if s * 4 // subs == p:
                    pump_a(k, s)
                    start_b(order(k), s)

    def back(k, p):
        @pl.when(k < seq_n)
        def _():
            for s in range(subs):
                if s * 4 // subs == p:
                    end_b(order(k), s)

    slots = 2 * tiles + 2

    def text_front(i, slot):
        last = seq_n - 1
        if slot == tiles:
            for d in (1, -1):

                @pl.when(jnp.logical_and(i == 1, inside(z + d)))
                def _():
                    first_t(d).start()

        if slot == 0 and last > 1:

            @pl.when(i == last)
            def _():
                pump_t(last - 1)

        if slot == tiles:

            @pl.when(jnp.logical_and(i > 1, i < last))
            def _():
                pump_t(i - 1)

        if slot == 2 * tiles - 1:

            @pl.when(i == last)
            def _():
                pump_t(last)

    def pump(i, slot):
        if slot == 0:
            front(i + 1, 2)
        if slot == min(2, 2 * tiles - 1):
            front(i + 1, 3)
        if slot == tiles:
            back(i + 1, 0)
        if slot == 2 * tiles - 1:
            back(i + 1, 1)
        if slot == 2 * tiles:
            back(i + 1, 2)
            front(i + 2, 0)
        if slot == slots - 1:
            back(i + 1, 3)
            front(i + 2, 1)
        text_front(i, slot)

    def project(j, t, b):
        at = pl.ds(t * tile, tile)
        return jnp.dot(
            mod[b * rows : (b + 1) * rows, :], wfull[j, :, at], preferred_element_type=F32
        )

    def finish(j, t, b, y):
        if j == 2:
            y = y.astype(BF16)
            for hh in range(per_tile):
                vbuf[b * heads + t * per_tile + hh] = y[:, hh * HEAD_DIM : (hh + 1) * HEAD_DIM]
            return
        swapped = jnp.dot(y.astype(BF16), mix[0, :tile, :tile], preferred_element_type=F32)
        square = jnp.dot((y * y).astype(BF16), mix[1, :tile, :tile], preferred_element_type=F32)
        inverse = lax.rsqrt(square + 1e-06)
        dest = kbuf if j == 1 else qbuf
        for hh in range(per_tile):
            at = slice(hh * HEAD_DIM, (hh + 1) * HEAD_DIM)
            turned = y[:, at] * tab[2 * j] + swapped[:, at] * tab[2 * j + 1]
            dest[b * heads + t * per_tile + hh] = (turned * inverse[:, at]).astype(BF16)

    def attend(span, first):
        ahead = {}
        for n in range(len(span) + 2):
            if n < len(span):
                h = span[n]
                ahead[n] = lax.dot_general(
                    qbuf[h], kbuf[h], (((1,), (1,)), ((), ())), preferred_element_type=F32
                )
            if n < 2:
                continue
            h = span[n - 2]
            expo = jnp.exp2(ahead.pop(n - 2))
            folded = expo[:, :HEAD_DIM]
            for k in range(1, rows // HEAD_DIM):
                folded = folded + expo[:, k * HEAD_DIM : (k + 1) * HEAD_DIM]
            mixed = jnp.dot(expo.astype(BF16), vbuf[h], preferred_element_type=F32)
            if first:
                lsum[h] = folded
                acc[h] = mixed
            else:
                lsum[h] += folded
                acc[h] += mixed

    def tables(o, first):
        place = lax.dot_general(
            pos[o], pick[...], (((0,), (0,)), ((), ())), preferred_element_type=F32
        )
        turns = place * rot[0:1, :]
        angle = (turns - jnp.floor(turns + 0.5)) * math.pi
        square = angle * angle
        low = angle * horner(SIN, square)
        cosine = 1.0 - 2.0 * low * low
        sine = 2.0 * low * horner(COS, square)
        for j in range(0 if first else 1, 2):
            strength = scale if j == 0 else 1.0
            tab[2 * j] = cosine * (gain_rows[j][0:1] * strength)
            tab[2 * j + 1] = sine * (gain_rows[j][1:2] * strength)

    swap_abs = jnp.abs(mix[0, :HEAD_DIM, :HEAD_DIM].astype(F32))
    gain_rows = []
    for j in range(2):
        own = gains[j : j + 1, :]
        column = jnp.sum(
            jnp.where(
                lax.broadcasted_iota(jnp.int32, (HEAD_DIM, HEAD_DIM), 0)
                == lax.broadcasted_iota(jnp.int32, (HEAD_DIM, HEAD_DIM), 1),
                own,
                0.0,
            ),
            axis=1,
            keepdims=True,
        )
        gain_rows.append(jnp.concatenate([own, jnp.sum(swap_abs * column, axis=0, keepdims=True)]))

    def modulate(o, core):
        @pl.loop(0, half_rows // STRIP, unroll=U_MOD)
        def _(r):
            start = aligned(core * (half_rows // STRIP) + r, STRIP)
            normed = lat[o, pl.ds(start, STRIP), :].astype(F32)
            for b in range(2):
                mod[pl.ds(pl.multiple_of(b * rows + start, STRIP), STRIP), :] = (
                    normed * (1.0 + modulation[1, b : b + 1, :]) + modulation[0, b : b + 1, :]
                ).astype(BF16)

    def step(i, first):
        o = order(i)
        tables(o, first)
        modulate(o, c)
        if not first:
            for s in range(subs):
                copy_c(o, s, other).wait_recv()
        modulate(o, other)

        pending = None
        for j in range(0 if first else 1, 3):
            if first:
                w_local[j].wait()
                w_copy[j].wait_recv()
            for t in range(tiles):
                for b in range(2):
                    y = project(j, t, b)
                    if pending is not None:
                        finish(*pending)
                    pending = (j, t, b, y)
                if j > 0:
                    pump(i, (j - 1) * tiles + t)
                    continue
                if t == max(tiles - 2, 0):
                    front(1, 0)
                if t == tiles - 1:
                    front(1, 1)
        finish(*pending)
        group = heads
        for g in range(2):
            attend(list(range(g * group, (g + 1) * group)), first)
            pump(i, 2 * tiles + g)

    step(0, True)

    @pl.loop(1, seq_n)
    def _(i):
        step(i, False)

    txt_local.wait()
    copy_l(other).wait_recv()

    @pl.loop(0, seq_n)
    def _(o):
        copy_u(o).wait_recv()

    text_rows = txt.shape[2]
    count = seq_n * text_rows

    def copy_o(core, t, own):
        to = (x + t) % ten_n
        branch = core if own == 0 else 1 - core
        at = pl.ds(aligned(branch, out_rows), out_rows)
        place = attf.at[core, to, at]
        return remote(place, place, send_o.at[t, own], recv_o.at[t, own], cfg=other)

    def text(t, own):
        to = (x + t) % ten_n
        here = pl.ds(aligned(to, out_rows), out_rows)
        branch = c if own == 0 else other
        source = txt if own == 0 else txo
        base = aligned(c, mine) if own == 0 else 0
        valid = lax.broadcasted_iota(jnp.int32, (1, count), 1).astype(F32) < lens[branch, 0:1, :]
        ahead = {}
        for n in range(heads + 2):
            if n < heads:
                src = pl.ds(pl.multiple_of(base + n * HEAD_DIM, HEAD_DIM), HEAD_DIM)
                raw = source[:, 0, :, src].reshape(count, HEAD_DIM).astype(F32)
                inverse = lax.rsqrt(jnp.mean(raw * raw, axis=-1, keepdims=True) + 1e-06)
                keys = (raw * inverse * gains[1:2, :]).astype(BF16)
                ahead[n] = lax.dot_general(
                    qbuf[branch * heads + n, here, :],
                    keys,
                    (((1,), (1,)), ((), ())),
                    preferred_element_type=F32,
                )
            if n < 2:
                continue
            h = n - 2
            row = branch * heads + h
            src = pl.ds(pl.multiple_of(base + h * HEAD_DIM, HEAD_DIM), HEAD_DIM)
            values = source[:, 1, :, src].reshape(count, HEAD_DIM)
            expo = jnp.where(valid, jnp.exp2(ahead.pop(h)), 0.0)
            total = jnp.sum(lsum[row, here, :], axis=-1, keepdims=True) + jnp.sum(
                expo, axis=-1, keepdims=True
            )
            mixed = acc[row, here, :] + jnp.dot(
                expo.astype(BF16), values, preferred_element_type=F32
            )
            attf[
                c, to, pl.ds(aligned(branch, out_rows), out_rows), h * HEAD_DIM : (h + 1) * HEAD_DIM
            ] = (mixed * (1.0 / total)).astype(BF16)
        copy_o(c, t, own).start()

    out_tile = 256 if out_cols % 256 == 0 else 128
    out_tiles = out_cols // out_tile

    def copy_r(t, k):
        return remote(
            part.at[t, k], got.at[t, k], send_r.at[t, k], recv_r.at[t, k], tensor=(x + t) % ten_n
        )

    strength = guide[0:1, 0:1]

    def out_block(t, k):
        to = (x + t) % ten_n
        at = pl.ds(k * out_tile, out_tile)
        y = jnp.dot(attf[0, to], wout[0:mine, at], preferred_element_type=F32)
        y = y + jnp.dot(attf[1, to], wout[mine : 2 * mine, at], preferred_element_type=F32)
        at_gate = pl.ds(pl.multiple_of(c * out_cols + k * out_tile, out_tile), out_tile)
        return (
            y[:out_rows] * (strength * modulation[2, 0:1, at_gate])
            + y[out_rows:] * ((1.0 - strength) * modulation[2, 1:2, at_gate])
        )

    turn = list(range(1, ten_n)) + [0]
    text(turn[0], 0)
    text(turn[0], 1)
    out_local.wait()
    for n, t in enumerate(turn):
        if n + 1 < ten_n:
            text(turn[n + 1], 0)
        copy_o(other, t, 0).wait_recv()
        copy_o(other, t, 1).wait_recv()
        block = out_block(t, 0)
        for k in range(out_tiles):
            later = out_block(t, k + 1) if k + 1 < out_tiles else None
            part[t, k] = block.astype(BF16)
            if t > 0:
                copy_r(t, k).start()
            block = later
        if n + 1 < ten_n:
            text(turn[n + 1], 1)

    for j in range(3):
        w_copy[j].wait_send()
    copy_l(c).wait_send()
    for t in range(ten_n):
        for own in range(2):
            copy_o(c, t, own).wait_send()

    @pl.loop(0, seq_n)
    def _(o):
        copy_u(o).wait_send()

        @pl.when(o != z)
        def _():
            for s in range(subs):
                for t in range(1, ten_n):
                    copy_b(o, s, t).wait_send()
                copy_c(o, s, c).wait_send()

        for d in (1, -1):
            ahead = jnp.logical_or(o == z, d * (z - o) > 0)

            @pl.when(jnp.logical_and(ahead, inside(z + d)))
            def _():
                copy_p(o, d).wait_send()
                copy_t(o, d).wait_send()
                for s in range(subs):
                    copy_a(o, s, d).wait_send()

    def emit(k):
        return pltpu.make_async_copy(
            part.at[0, k], out.at[:, pl.ds(k * out_tile, out_tile)], loc.at[8 + k]
        )

    for k in range(out_tiles):
        total = part[0, k].astype(F32)
        for t in range(1, ten_n):
            copy_r(t, k).wait_recv()
            total = total + got[t, k].astype(F32)
        part[0, k] = total.astype(BF16)
        emit(k).start()
    for k in range(out_tiles):
        for t in range(1, ten_n):
            copy_r(t, k).wait_send()
        emit(k).wait()


def local(
    seq_n, ten_n, latent, positions, text_kv, text_len, modulation, w_qkv, norm_gains, w_out, guidance
):
    rows, width = latent.shape
    mine = w_qkv.shape[2] // 2
    heads = mine // HEAD_DIM
    text_dev = text_kv.shape[2]
    out_rows = rows // ten_n
    out_cols = w_out.shape[1]
    out_tile = 256 if out_cols % 256 == 0 else 128
    out_tiles = out_cols // out_tile
    subs = rows // (2 * ten_n * STRIP)
    any_space = pl.BlockSpec(memory_space=pl.ANY)
    vmem = pl.BlockSpec(memory_space=pltpu.VMEM)
    dma = pltpu.SemaphoreType.DMA
    return pl.pallas_call(
        functools.partial(kernel, seq_n, ten_n),
        out_shape=jax.ShapeDtypeStruct((out_rows, out_cols), BF16),
        in_specs=[
            any_space,
            vmem,
            any_space,
            vmem,
            vmem,
            any_space,
            vmem,
            any_space,
            vmem,
            vmem,
            vmem,
            vmem,
        ],
        out_specs=any_space,
        scratch_shapes=[
            pltpu.VMEM((seq_n, rows, width), BF16),
            pltpu.VMEM((seq_n, 16, rows), BF16),
            pltpu.VMEM((seq_n, 2, text_dev, 2 * mine), BF16),
            pltpu.VMEM((seq_n, 2, text_dev, mine), BF16),
            pltpu.VMEM((2, 8, seq_n * text_dev), F32),
            pltpu.VMEM((3, width, mine), BF16),
            pltpu.VMEM(w_out.shape, BF16),
            pltpu.VMEM((2 * rows, width), BF16),
            pltpu.VMEM((4, rows, HEAD_DIM), F32),
            pltpu.VMEM((2 * heads, rows, HEAD_DIM), BF16),
            pltpu.VMEM((2 * heads, rows, HEAD_DIM), BF16),
            pltpu.VMEM((2 * heads, rows, HEAD_DIM), BF16),
            pltpu.VMEM((2 * heads, rows, HEAD_DIM), F32),
            pltpu.VMEM((2 * heads, rows, HEAD_DIM), F32),
            pltpu.VMEM((2, ten_n, 2 * out_rows, mine), BF16),
            pltpu.VMEM((ten_n, out_tiles, out_rows, out_tile), BF16),
            pltpu.VMEM((ten_n, out_tiles, out_rows, out_tile), BF16),
            dma((seq_n, subs, 2)),
            dma((seq_n, subs)),
            dma((seq_n, subs, ten_n)),
            dma((seq_n, subs, ten_n)),
            dma((seq_n, subs)),
            dma((seq_n, subs)),
            dma((seq_n, 2)),
            dma((seq_n,)),
            dma((seq_n, 2)),
            dma((seq_n,)),
            dma((seq_n,)),
            dma((seq_n,)),
            dma((3,)),
            dma((3,)),
            dma((1,)),
            dma((1,)),
            dma((ten_n, 2)),
            dma((ten_n, 2)),
            dma((ten_n, out_tiles)),
            dma((ten_n, out_tiles)),
            dma((8 + out_tiles,)),
        ],
        compiler_params=pltpu.CompilerParams(
            collective_id=0, has_side_effects=True, vmem_limit_bytes=64 * 1024 * 1024 - 65536
        ),
    )(
        latent,
        positions,
        text_kv,
        text_len.reshape(1, 1),
        modulation,
        w_qkv,
        norm_gains,
        w_out,
        guidance.reshape(1, 1),
        jnp.asarray(ROT_ROWS),
        jnp.asarray(ROT_PICK, BF16),
        jnp.asarray(MIX, BF16),
    )


def solution(mesh):
    placed = (
        P(("groups", "seq"), None),
        P(None, ("groups", "seq")),
        P("cfg", None, ("groups", "seq"), "tensor"),
        P(("groups", "cfg")),
        P(None, "groups", None),
        P(None, "cfg", "tensor"),
        P(),
        P("tensor", "cfg"),
        P("groups"),
    )
    return jax.shard_map(
        functools.partial(local, mesh.shape["seq"], mesh.shape["tensor"]),
        mesh=mesh,
        in_specs=placed,
        out_specs=P(("groups", "seq", "tensor"), "cfg"),
        check_vma=False,
    )
```

```python
import functools
import math

import jax
import jax.numpy as jnp
import numpy as np
from jax import lax
from jax.experimental import pallas as pl
from jax.experimental.pallas import tpu as pltpu
from jax.sharding import PartitionSpec as P

HEAD_DIM = 128
MESH = pl.DeviceIdType.MESH
U_MOD = 8
F32 = jnp.float32
BF16 = jnp.bfloat16


def rotary_rows(head_size):
    rows = np.zeros((8, head_size), np.float32)
    swap = np.zeros((head_size, head_size), np.float32)
    axes = np.zeros((head_size,), np.int32)
    blocks = (head_size // 8, 7 * head_size // 16, 7 * head_size // 16)
    offset = 0
    for axis_id, width in enumerate(blocks):
        half = width // 2
        turns = 256.0 ** (-np.arange(half, dtype=np.float64) / half) / (2 * np.pi)
        rows[0, offset : offset + half] = turns
        rows[0, offset + half : offset + width] = turns
        for k in range(half):
            swap[offset + half + k, offset + k] = -1.0
            swap[offset + k, offset + half + k] = 1.0
        axes[offset : offset + width] = axis_id
        offset += width
    return rows, axes, swap


ROT_ROWS, ROT_AXES, ROT_SWAP = rotary_rows(HEAD_DIM)
ROT_PICK = (np.arange(16)[:, None] == ROT_AXES[None, :]).astype(np.float32)
SIDE = np.kron(np.eye(2), np.ones((HEAD_DIM, HEAD_DIM)))
MIX = np.stack([np.kron(np.eye(2), ROT_SWAP), SIDE / HEAD_DIM]).astype(np.float32)
SIN = tuple((-1.0) ** k / math.factorial(2 * k + 1) for k in range(6))
COS = tuple((-1.0) ** k / math.factorial(2 * k) for k in range(6))
LOG2E = 1.4426950408889634


def horner(terms, value):
    total = terms[-1]
    for term in terms[-2::-1]:
        total = total * value + term
    return total


STRIP = 16


def kernel(
    seq_n,
    ten_n,
    latent,
    pos_in,
    text_kv,
    lens_in,
    modulation,
    w_qkv,
    gains,
    w_out,
    guide,
    rot,
    pick,
    mix,
    out,
    lat,
    pos,
    txt,
    txo,
    lens,
    wfull,
    wout,
    mod,
    tab,
    qbuf,
    kbuf,
    vbuf,
    acc,
    lsum,
    attf,
    part,
    got,
    send_a,
    recv_a,
    send_b,
    recv_b,
    send_c,
    recv_c,
    send_p,
    recv_p,
    send_t,
    recv_t,
    send_u,
    recv_u,
    send_w,
    recv_w,
    send_l,
    recv_l,
    send_o,
    recv_o,
    send_r,
    recv_r,
    loc,
):
    x = lax.axis_index("tensor")
    c = lax.axis_index("cfg")
    z = lax.axis_index("seq")
    other = 1 - c
    rows, width = latent.shape
    half = w_qkv.shape[1]
    mine = wfull.shape[2]
    heads = mine // HEAD_DIM
    half_rows = rows // 2
    band = ten_n * STRIP
    subs = half_rows // band
    out_rows = rows // ten_n
    out_cols = w_out.shape[1]
    scale = HEAD_DIM ** (-0.5) * LOG2E
    tile = 256 if mine % 256 == 0 else 128
    per_tile = tile // HEAD_DIM
    tiles = mine // tile
    shorter = jnp.minimum(z, seq_n - 1 - z)
    long_sign = jnp.where(2 * z < seq_n - 1, 1, -1)

    def order(i):
        near = i <= 2 * shorter
        dist = jnp.where(near, (i + 1) // 2, i - shorter)
        sign = jnp.where(near, 2 * (i % 2) - 1, long_sign)
        return jnp.where(i == 0, z, z + dist * sign)

    def remote(src, dst, send, recv, **to):
        return pltpu.make_async_remote_copy(
            src_ref=src, dst_ref=dst, send_sem=send, recv_sem=recv, device_id=to, device_id_type=MESH
        )

    def aligned(value, unit):
        return pl.multiple_of(value * unit, unit)

    def inside(o):
        return jnp.logical_and(o >= 0, o < seq_n)

    cols_of = lambda core: pl.ds(aligned(core, mine), mine)
    w_copy = [
        remote(
            w_qkv.at[j, :, cols_of(other)],
            wfull.at[j, pl.ds(aligned(c, half), half), :],
            send_w.at[j],
            recv_w.at[j],
            cfg=other,
        )
        for j in range(3)
    ]
    w_local = [
        pltpu.make_async_copy(
            w_qkv.at[j, :, cols_of(c)], wfull.at[j, pl.ds(aligned(c, half), half), :], loc.at[j]
        )
        for j in range(3)
    ]
    lat_local = pltpu.make_async_copy(latent, lat.at[z], loc.at[3])
    txt_local = pltpu.make_async_copy(text_kv.at[0], txt.at[z], loc.at[5])
    out_local = pltpu.make_async_copy(w_out, wout, loc.at[7])

    def strip_of(core, s, ten):
        return pl.ds(aligned((core * subs + s) * ten_n + ten, STRIP), STRIP)

    def band_of(core, s):
        return pl.ds(aligned(core * subs + s, band), band)

    def up(d):
        return 0 if d > 0 else 1

    def copy_a(o, s, d):
        at = strip_of(c, s, x)
        return remote(lat.at[o, at], lat.at[o, at], send_a.at[o, s, up(d)], recv_a.at[o, s], seq=z + d)

    def copy_b(o, s, t):
        at = strip_of(c, s, x)
        to = (x + t) % ten_n
        return remote(lat.at[o, at], lat.at[o, at], send_b.at[o, s, t - 1], recv_b.at[o, s, t - 1], tensor=to)

    def arrived_b(o, s, t):
        source = (x + ten_n - t) % ten_n
        at = strip_of(c, s, source)
        return remote(lat.at[o, at], lat.at[o, at], send_b.at[o, s, t - 1], recv_b.at[o, s, t - 1], tensor=source)

    def copy_c(o, s, core):
        at = band_of(core, s)
        return remote(lat.at[o, at], lat.at[o, at], send_c.at[o, s], recv_c.at[o, s], cfg=other)

    def first_p(d):
        return copy_p(z, d)

    def copy_p(o, d):
        return remote(pos.at[o], pos.at[o], send_p.at[o, up(d)], recv_p.at[o], seq=z + d)

    def first_t(d):
        return remote(text_kv.at[0], txt.at[z], send_t.at[z, up(d)], recv_t.at[z], seq=z + d)

    def copy_t(o, d):
        return remote(txt.at[o], txt.at[o], send_t.at[o, up(d)], recv_t.at[o], seq=z + d)

    def first_u():
        return remote(
            text_kv.at[0, :, :, cols_of(other)], txo.at[z], send_u.at[z], recv_u.at[z], cfg=other
        )

    def copy_u(o):
        return remote(txt.at[o, :, :, cols_of(other)], txo.at[o], send_u.at[o], recv_u.at[o], cfg=other)

    def copy_l(core):
        return remote(lens.at[core], lens.at[core], send_l.at[0], recv_l.at[0], cfg=other)

    lat_local.start()

    barrier = pltpu.get_barrier_semaphore()
    for d in (1, -1):

        @pl.when(inside(z + d))
        def _():
            pl.semaphore_signal(barrier, inc=1, device_id={"seq": z + d}, device_id_type=MESH)

    pl.semaphore_signal(barrier, inc=1, device_id={"cfg": other}, device_id_type=MESH)
    for t in range(1, ten_n):
        pl.semaphore_signal(
            barrier, inc=1, device_id={"tensor": (x + t) % ten_n}, device_id_type=MESH
        )

    def normalize(core, ten):
        spots = [strip_of(core, s, ten) for s in range(subs)]
        lanes = [slice(k * HEAD_DIM, (k + 1) * HEAD_DIM) for k in range(width // HEAD_DIM)]

        def mean_of(body):
            means = []
            for at in spots:
                total = body(at, lanes[0], len(means))
                for lane in lanes[1:]:
                    total = total + body(at, lane, len(means))
                means.append(jnp.sum(total, axis=-1, keepdims=True) * (1.0 / width))
            return means

        means = mean_of(lambda at, lane, n: lat[z, at, lane].astype(F32))

        def squared(at, lane, n):
            center = lat[z, at, lane].astype(F32) - means[n]
            return center * center

        inverses = [lax.rsqrt(power + 1e-06) for power in mean_of(squared)]
        for n, at in enumerate(spots):
            for lane in lanes:
                lat[z, at, lane] = (
                    (lat[z, at, lane].astype(F32) - means[n]) * inverses[n]
                ).astype(BF16)

    pos[z] = jnp.concatenate(
        [pos_in[...].astype(F32), jnp.zeros((16 - pos_in.shape[0], rows), F32)]
    ).astype(BF16)
    lens[c] = jnp.broadcast_to(lens_in[0:1, 0:1].astype(F32), lens.shape[1:])
    lat_local.wait()
    for j in range(3):
        w_local[j].start()
    txt_local.start()
    out_local.start()
    normalize(c, x)

    sides = jnp.where(z > 0, 1, 0) + jnp.where(z < seq_n - 1, 1, 0)
    pl.semaphore_wait(barrier, ten_n + sides)

    for d in (1, -1):

        @pl.when(inside(z + d))
        def _():
            first_p(d).start()
            for s in range(subs):
                copy_a(z, s, d).start()

    for j in range(3):
        w_copy[j].start()
    copy_l(c).start()
    first_u().start()

    @pl.loop(1, 2 * ten_n)
    def _(g):
        normalize(jnp.where(g < ten_n, c, other), (x + g) % ten_n)

    def pump_a(k, s):
        for d in (1, -1):
            o = z - d * k

            @pl.when(inside(o))
            def _():
                if s == 0:
                    copy_p(o, d).wait_recv()
                copy_a(o, s, d).wait_recv()

                @pl.when(inside(z + d))
                def _():
                    if s == 0:
                        copy_p(o, d).start()
                    copy_a(o, s, d).start()

    def pump_t(k):
        for d in (1, -1):
            o = z - d * k

            @pl.when(inside(o))
            def _():
                copy_t(o, d).wait_recv()

                @pl.when(inside(z + d))
                def _():
                    copy_t(o, d).start()

                copy_u(o).start()

    def start_b(o, s):
        for t in range(1, ten_n):
            copy_b(o, s, t).start()

    def end_b(o, s):
        for t in range(1, ten_n):
            arrived_b(o, s, t).wait_recv()
        copy_c(o, s, c).start()

    def front(k, p):
        @pl.when(k < seq_n)
        def _():
            for s in range(subs):
                if s * 4 // subs == p:
                    pump_a(k, s)
                    start_b(order(k), s)

    def back(k, p):
        @pl.when(k < seq_n)
        def _():
            for s in range(subs):
                if s * 4 // subs == p:
                    end_b(order(k), s)

    slots = 2 * tiles + 2

    def text_front(i, slot):
        last = seq_n - 1
        if slot == tiles:
            for d in (1, -1):

                @pl.when(jnp.logical_and(i == 1, inside(z + d)))
                def _():
                    first_t(d).start()

        if slot == 0 and last > 1:

            @pl.when(i == last)
            def _():
                pump_t(last - 1)

        if slot == tiles:

            @pl.when(jnp.logical_and(i > 1, i < last))
            def _():
                pump_t(i - 1)

        if slot == 2 * tiles - 1:

            @pl.when(i == last)
            def _():
                pump_t(last)

    def pump(i, slot):
        if slot == 0:
            front(i + 1, 2)
        if slot == min(2, 2 * tiles - 1):
            front(i + 1, 3)
        if slot == tiles:
            back(i + 1, 0)
        if slot == 2 * tiles - 1:
            back(i + 1, 1)
        if slot == 2 * tiles:
            back(i + 1, 2)
            front(i + 2, 0)
        if slot == slots - 1:
            back(i + 1, 3)
            front(i + 2, 1)
        text_front(i, slot)

    def project(j, t, b):
        at = pl.ds(t * tile, tile)
        return jnp.dot(
            mod[b * rows : (b + 1) * rows, :], wfull[j, :, at], preferred_element_type=F32
        )

    def finish(j, t, b, y):
        if j == 2:
            y = y.astype(BF16)
            for hh in range(per_tile):
                vbuf[b * heads + t * per_tile + hh] = y[:, hh * HEAD_DIM : (hh + 1) * HEAD_DIM]
            return
        swapped = jnp.dot(y.astype(BF16), mix[0, :tile, :tile], preferred_element_type=F32)
        square = jnp.dot((y * y).astype(BF16), mix[1, :tile, :tile], preferred_element_type=F32)
        inverse = lax.rsqrt(square + 1e-06)
        dest = kbuf if j == 1 else qbuf
        for hh in range(per_tile):
            at = slice(hh * HEAD_DIM, (hh + 1) * HEAD_DIM)
            turned = y[:, at] * tab[2 * j] + swapped[:, at] * tab[2 * j + 1]
            dest[b * heads + t * per_tile + hh] = (turned * inverse[:, at]).astype(BF16)

    def attend(span, first):
        ahead = {}
        for n in range(len(span) + 2):
            if n < len(span):
                h = span[n]
                ahead[n] = lax.dot_general(
                    qbuf[h], kbuf[h], (((1,), (1,)), ((), ())), preferred_element_type=F32
                )
            if n < 2:
                continue
            h = span[n - 2]
            expo = jnp.exp2(ahead.pop(n - 2))
            folded = expo[:, :HEAD_DIM]
            for k in range(1, rows // HEAD_DIM):
                folded = folded + expo[:, k * HEAD_DIM : (k + 1) * HEAD_DIM]
            mixed = jnp.dot(expo.astype(BF16), vbuf[h], preferred_element_type=F32)
            if first:
                lsum[h] = folded
                acc[h] = mixed
            else:
                lsum[h] += folded
                acc[h] += mixed

    def tables(o, first):
        place = lax.dot_general(
            pos[o], pick[...], (((0,), (0,)), ((), ())), preferred_element_type=F32
        )
        turns = place * rot[0:1, :]
        angle = (turns - jnp.floor(turns + 0.5)) * math.pi
        square = angle * angle
        low = angle * horner(SIN, square)
        cosine = 1.0 - 2.0 * low * low
        sine = 2.0 * low * horner(COS, square)
        for j in range(0 if first else 1, 2):
            strength = scale if j == 0 else 1.0
            tab[2 * j] = cosine * (gain_rows[j][0:1] * strength)
            tab[2 * j + 1] = sine * (gain_rows[j][1:2] * strength)

    swap_abs = jnp.abs(mix[0, :HEAD_DIM, :HEAD_DIM].astype(F32))
    gain_rows = []
    for j in range(2):
        own = gains[j : j + 1, :]
        column = jnp.sum(
            jnp.where(
                lax.broadcasted_iota(jnp.int32, (HEAD_DIM, HEAD_DIM), 0)
                == lax.broadcasted_iota(jnp.int32, (HEAD_DIM, HEAD_DIM), 1),
                own,
                0.0,
            ),
            axis=1,
            keepdims=True,
        )
        gain_rows.append(jnp.concatenate([own, jnp.sum(swap_abs * column, axis=0, keepdims=True)]))

    def modulate(o, core):
        @pl.loop(0, half_rows // STRIP, unroll=U_MOD)
        def _(r):
            start = aligned(core * (half_rows // STRIP) + r, STRIP)
            normed = lat[o, pl.ds(start, STRIP), :].astype(F32)
            for b in range(2):
                mod[pl.ds(pl.multiple_of(b * rows + start, STRIP), STRIP), :] = (
                    normed * (1.0 + modulation[1, b : b + 1, :]) + modulation[0, b : b + 1, :]
                ).astype(BF16)

    def step(i, first):
        o = order(i)
        tables(o, first)
        modulate(o, c)
        if not first:
            for s in range(subs):
                copy_c(o, s, other).wait_recv()
        modulate(o, other)

        pending = None
        for j in range(0 if first else 1, 3):
            if first:
                w_local[j].wait()
                w_copy[j].wait_recv()
            for t in range(tiles):
                for b in range(2):
                    y = project(j, t, b)
                    if pending is not None:
                        finish(*pending)
                    pending = (j, t, b, y)
                if j > 0:
                    pump(i, (j - 1) * tiles + t)
                    continue
                if t == 0:
                    front(1, 0)
                if t == tiles - 1:
                    front(1, 1)
        finish(*pending)
        group = heads
        for g in range(2):
            attend(list(range(g * group, (g + 1) * group)), first)
            pump(i, 2 * tiles + g)

    step(0, True)

    @pl.loop(1, seq_n)
    def _(i):
        step(i, False)

    txt_local.wait()
    copy_l(other).wait_recv()

    @pl.loop(0, seq_n)
    def _(o):
        copy_u(o).wait_recv()

    text_rows = txt.shape[2]
    count = seq_n * text_rows

    def copy_o(core, t, own):
        to = (x + t) % ten_n
        branch = core if own == 0 else 1 - core
        at = pl.ds(aligned(branch, out_rows), out_rows)
        place = attf.at[core, to, at]
        return remote(place, place, send_o.at[t, own], recv_o.at[t, own], cfg=other)

    def text(t, own):
        to = (x + t) % ten_n
        here = pl.ds(aligned(to, out_rows), out_rows)
        branch = c if own == 0 else other
        source = txt if own == 0 else txo
        base = aligned(c, mine) if own == 0 else 0
        valid = lax.broadcasted_iota(jnp.int32, (1, count), 1).astype(F32) < lens[branch, 0:1, :]
        ahead = {}
        for n in range(heads + 2):
            if n < heads:
                src = pl.ds(pl.multiple_of(base + n * HEAD_DIM, HEAD_DIM), HEAD_DIM)
                raw = source[:, 0, :, src].reshape(count, HEAD_DIM).astype(F32)
                inverse = lax.rsqrt(jnp.mean(raw * raw, axis=-1, keepdims=True) + 1e-06)
                keys = (raw * inverse * gains[1:2, :]).astype(BF16)
                ahead[n] = lax.dot_general(
                    qbuf[branch * heads + n, here, :],
                    keys,
                    (((1,), (1,)), ((), ())),
                    preferred_element_type=F32,
                )
            if n < 2:
                continue
            h = n - 2
            row = branch * heads + h
            src = pl.ds(pl.multiple_of(base + h * HEAD_DIM, HEAD_DIM), HEAD_DIM)
            values = source[:, 1, :, src].reshape(count, HEAD_DIM)
            expo = jnp.where(valid, jnp.exp2(ahead.pop(h)), 0.0)
            total = jnp.sum(lsum[row, here, :], axis=-1, keepdims=True) + jnp.sum(
                expo, axis=-1, keepdims=True
            )
            mixed = acc[row, here, :] + jnp.dot(
                expo.astype(BF16), values, preferred_element_type=F32
            )
            attf[
                c, to, pl.ds(aligned(branch, out_rows), out_rows), h * HEAD_DIM : (h + 1) * HEAD_DIM
            ] = (mixed * (1.0 / total)).astype(BF16)
        copy_o(c, t, own).start()

    out_tile = 256 if out_cols % 256 == 0 else 128
    out_tiles = out_cols // out_tile

    def copy_r(t, k):
        return remote(
            part.at[t, k], got.at[t, k], send_r.at[t, k], recv_r.at[t, k], tensor=(x + t) % ten_n
        )

    strength = guide[0:1, 0:1]

    def out_block(t, k):
        to = (x + t) % ten_n
        at = pl.ds(aligned(k, out_tile), out_tile)
        y = jnp.dot(attf[0, to], wout[0:mine, at], preferred_element_type=F32)
        y = y + jnp.dot(attf[1, to], wout[mine : 2 * mine, at], preferred_element_type=F32)
        at_gate = pl.ds(pl.multiple_of(c * out_cols + k * out_tile, out_tile), out_tile)
        return (
            y[:out_rows] * (strength * modulation[2, 0:1, at_gate])
            + y[out_rows:] * ((1.0 - strength) * modulation[2, 1:2, at_gate])
        )

    turn = list(range(1, ten_n)) + [0]
    text(turn[0], 0)
    text(turn[0], 1)
    out_local.wait()
    for n, t in enumerate(turn):
        if n + 1 < ten_n:
            text(turn[n + 1], 0)
        copy_o(other, t, 0).wait_recv()
        copy_o(other, t, 1).wait_recv()
        if t > 0:

            @pl.loop(0, out_tiles)
            def _(k):
                part[t, k] = out_block(t, k).astype(BF16)
                copy_r(t, k).start()

        else:
            for k in range(out_tiles):
                part[t, k] = out_block(t, k).astype(BF16)
        if n + 1 < ten_n:
            text(turn[n + 1], 1)

    for j in range(3):
        w_copy[j].wait_send()
    copy_l(c).wait_send()
    for t in range(ten_n):
        for own in range(2):
            copy_o(c, t, own).wait_send()

    @pl.loop(0, seq_n)
    def _(o):
        copy_u(o).wait_send()

        @pl.when(o != z)
        def _():
            for s in range(subs):
                for t in range(1, ten_n):
                    copy_b(o, s, t).wait_send()
                copy_c(o, s, c).wait_send()

        for d in (1, -1):
            ahead = jnp.logical_or(o == z, d * (z - o) > 0)

            @pl.when(jnp.logical_and(ahead, inside(z + d)))
            def _():
                copy_p(o, d).wait_send()
                copy_t(o, d).wait_send()
                for s in range(subs):
                    copy_a(o, s, d).wait_send()

    def emit(k):
        return pltpu.make_async_copy(
            part.at[0, k], out.at[:, pl.ds(k * out_tile, out_tile)], loc.at[8 + k]
        )

    for k in range(out_tiles):
        total = part[0, k].astype(F32)
        for t in range(1, ten_n):
            copy_r(t, k).wait_recv()
            total = total + got[t, k].astype(F32)
        part[0, k] = total.astype(BF16)
        emit(k).start()
    for k in range(out_tiles):
        for t in range(1, ten_n):
            copy_r(t, k).wait_send()
        emit(k).wait()


def local(
    seq_n, ten_n, latent, positions, text_kv, text_len, modulation, w_qkv, norm_gains, w_out, guidance
):
    rows, width = latent.shape
    mine = w_qkv.shape[2] // 2
    heads = mine // HEAD_DIM
    text_dev = text_kv.shape[2]
    out_rows = rows // ten_n
    out_cols = w_out.shape[1]
    out_tile = 256 if out_cols % 256 == 0 else 128
    out_tiles = out_cols // out_tile
    subs = rows // (2 * ten_n * STRIP)
    any_space = pl.BlockSpec(memory_space=pl.ANY)
    vmem = pl.BlockSpec(memory_space=pltpu.VMEM)
    dma = pltpu.SemaphoreType.DMA
    return pl.pallas_call(
        functools.partial(kernel, seq_n, ten_n),
        out_shape=jax.ShapeDtypeStruct((out_rows, out_cols), BF16),
        in_specs=[
            any_space,
            vmem,
            any_space,
            vmem,
            vmem,
            any_space,
            vmem,
            any_space,
            vmem,
            vmem,
            vmem,
            vmem,
        ],
        out_specs=any_space,
        scratch_shapes=[
            pltpu.VMEM((seq_n, rows, width), BF16),
            pltpu.VMEM((seq_n, 16, rows), BF16),
            pltpu.VMEM((seq_n, 2, text_dev, 2 * mine), BF16),
            pltpu.VMEM((seq_n, 2, text_dev, mine), BF16),
            pltpu.VMEM((2, 8, seq_n * text_dev), F32),
            pltpu.VMEM((3, width, mine), BF16),
            pltpu.VMEM(w_out.shape, BF16),
            pltpu.VMEM((2 * rows, width), BF16),
            pltpu.VMEM((4, rows, HEAD_DIM), F32),
            pltpu.VMEM((2 * heads, rows, HEAD_DIM), BF16),
            pltpu.VMEM((2 * heads, rows, HEAD_DIM), BF16),
            pltpu.VMEM((2 * heads, rows, HEAD_DIM), BF16),
            pltpu.VMEM((2 * heads, rows, HEAD_DIM), F32),
            pltpu.VMEM((2 * heads, rows, HEAD_DIM), F32),
            pltpu.VMEM((2, ten_n, 2 * out_rows, mine), BF16),
            pltpu.VMEM((ten_n, out_tiles, out_rows, out_tile), BF16),
            pltpu.VMEM((ten_n, out_tiles, out_rows, out_tile), BF16),
            dma((seq_n, subs, 2)),
            dma((seq_n, subs)),
            dma((seq_n, subs, max(ten_n - 1, 1))),
            dma((seq_n, subs, max(ten_n - 1, 1))),
            dma((seq_n, subs)),
            dma((seq_n, subs)),
            dma((seq_n, 2)),
            dma((seq_n,)),
            dma((seq_n, 2)),
            dma((seq_n,)),
            dma((seq_n,)),
            dma((seq_n,)),
            dma((3,)),
            dma((3,)),
            dma((1,)),
            dma((1,)),
            dma((ten_n, 2)),
            dma((ten_n, 2)),
            dma((ten_n, out_tiles)),
            dma((ten_n, out_tiles)),
            dma((8 + out_tiles,)),
        ],
        compiler_params=pltpu.CompilerParams(
            collective_id=0, has_side_effects=True, vmem_limit_bytes=64 * 1024 * 1024 - 65536
        ),
    )(
        latent,
        positions,
        text_kv,
        text_len.reshape(1, 1),
        modulation,
        w_qkv,
        norm_gains,
        w_out,
        guidance.reshape(1, 1),
        jnp.asarray(ROT_ROWS),
        jnp.asarray(ROT_PICK, BF16),
        jnp.asarray(MIX, BF16),
    )


def solution(mesh):
    placed = (
        P(("groups", "seq"), None),
        P(None, ("groups", "seq")),
        P("cfg", None, ("groups", "seq"), "tensor"),
        P(("groups", "cfg")),
        P(None, "groups", None),
        P(None, "cfg", "tensor"),
        P(),
        P("tensor", "cfg"),
        P("groups"),
    )
    return jax.shard_map(
        functools.partial(local, mesh.shape["seq"], mesh.shape["tensor"]),
        mesh=mesh,
        in_specs=placed,
        out_specs=P(("groups", "seq", "tensor"), "cfg"),
        check_vma=False,
    )
```

```python
import functools
import math

import jax
import jax.numpy as jnp
import numpy as np
from jax import lax
from jax.experimental import pallas as pl
from jax.experimental.pallas import tpu as pltpu
from jax.sharding import PartitionSpec as P

HEAD_DIM = 128
MESH = pl.DeviceIdType.MESH
U_MOD = 8
F32 = jnp.float32
BF16 = jnp.bfloat16


def rotary_rows(head_size):
    rows = np.zeros((8, head_size), np.float32)
    swap = np.zeros((head_size, head_size), np.float32)
    axes = np.zeros((head_size,), np.int32)
    blocks = (head_size // 8, 7 * head_size // 16, 7 * head_size // 16)
    offset = 0
    for axis_id, width in enumerate(blocks):
        half = width // 2
        turns = 256.0 ** (-np.arange(half, dtype=np.float64) / half) / (2 * np.pi)
        rows[0, offset : offset + half] = turns
        rows[0, offset + half : offset + width] = turns
        for k in range(half):
            swap[offset + half + k, offset + k] = -1.0
            swap[offset + k, offset + half + k] = 1.0
        axes[offset : offset + width] = axis_id
        offset += width
    return rows, axes, swap


ROT_ROWS, ROT_AXES, ROT_SWAP = rotary_rows(HEAD_DIM)
ROT_PICK = (np.arange(16)[:, None] == ROT_AXES[None, :]).astype(np.float32)
SIDE = np.kron(np.eye(2), np.ones((HEAD_DIM, HEAD_DIM)))
MIX = np.stack([np.kron(np.eye(2), ROT_SWAP), SIDE / HEAD_DIM]).astype(np.float32)
SIN = tuple((-1.0) ** k / math.factorial(2 * k + 1) for k in range(6))
COS = tuple((-1.0) ** k / math.factorial(2 * k) for k in range(6))
LOG2E = 1.4426950408889634


def horner(terms, value):
    total = terms[-1]
    for term in terms[-2::-1]:
        total = total * value + term
    return total


STRIP = 16


def kernel(
    seq_n,
    ten_n,
    latent,
    pos_in,
    text_kv,
    lens_in,
    modulation,
    w_qkv,
    gains,
    w_out,
    guide,
    rot,
    pick,
    mix,
    out,
    lat,
    pos,
    txt,
    txo,
    lens,
    wfull,
    wout,
    mod,
    tab,
    qbuf,
    kbuf,
    vbuf,
    acc,
    lsum,
    attf,
    part,
    got,
    send_a,
    recv_a,
    send_b,
    recv_b,
    send_c,
    recv_c,
    send_p,
    recv_p,
    send_t,
    recv_t,
    send_u,
    recv_u,
    send_w,
    recv_w,
    send_l,
    recv_l,
    send_o,
    recv_o,
    send_r,
    recv_r,
    loc,
):
    x = lax.axis_index("tensor")
    c = lax.axis_index("cfg")
    z = lax.axis_index("seq")
    other = 1 - c
    rows, width = latent.shape
    half = w_qkv.shape[1]
    mine = wfull.shape[2]
    heads = mine // HEAD_DIM
    half_rows = rows // 2
    band = ten_n * STRIP
    subs = half_rows // band
    out_rows = rows // ten_n
    out_cols = w_out.shape[1]
    scale = HEAD_DIM ** (-0.5) * LOG2E
    tile = 256 if mine % 256 == 0 else 128
    per_tile = tile // HEAD_DIM
    tiles = mine // tile
    shorter = jnp.minimum(z, seq_n - 1 - z)
    long_sign = jnp.where(2 * z < seq_n - 1, 1, -1)

    def order(i):
        near = i <= 2 * shorter
        dist = jnp.where(near, (i + 1) // 2, i - shorter)
        sign = jnp.where(near, 2 * (i % 2) - 1, long_sign)
        return jnp.where(i == 0, z, z + dist * sign)

    def remote(src, dst, send, recv, **to):
        return pltpu.make_async_remote_copy(
            src_ref=src, dst_ref=dst, send_sem=send, recv_sem=recv, device_id=to, device_id_type=MESH
        )

    def aligned(value, unit):
        return pl.multiple_of(value * unit, unit)

    def inside(o):
        return jnp.logical_and(o >= 0, o < seq_n)

    cols_of = lambda core: pl.ds(aligned(core, mine), mine)
    w_copy = [
        remote(
            w_qkv.at[j, :, cols_of(other)],
            wfull.at[j, pl.ds(aligned(c, half), half), :],
            send_w.at[j],
            recv_w.at[j],
            cfg=other,
        )
        for j in range(3)
    ]
    w_local = [
        pltpu.make_async_copy(
            w_qkv.at[j, :, cols_of(c)], wfull.at[j, pl.ds(aligned(c, half), half), :], loc.at[j]
        )
        for j in range(3)
    ]
    lat_local = pltpu.make_async_copy(latent, lat.at[z], loc.at[3])
    txt_local = pltpu.make_async_copy(text_kv.at[0], txt.at[z], loc.at[5])
    out_local = pltpu.make_async_copy(w_out, wout, loc.at[7])

    def strip_of(core, s, ten):
        return pl.ds(aligned((core * subs + s) * ten_n + ten, STRIP), STRIP)

    def band_of(core, s):
        return pl.ds(aligned(core * subs + s, band), band)

    def up(d):
        return 0 if d > 0 else 1

    def copy_a(o, s, d):
        at = strip_of(c, s, x)
        return remote(lat.at[o, at], lat.at[o, at], send_a.at[o, up(d)], recv_a.at[o, s], seq=z + d)

    def copy_b(o, s, t):
        at = strip_of(c, s, x)
        to = (x + t) % ten_n
        return remote(lat.at[o, at], lat.at[o, at], send_b.at[o, t - 1], recv_b.at[o, s, t - 1], tensor=to)

    def arrived_b(o, s, t):
        source = (x + ten_n - t) % ten_n
        at = strip_of(c, s, source)
        return remote(lat.at[o, at], lat.at[o, at], send_b.at[o, t - 1], recv_b.at[o, s, t - 1], tensor=source)

    def copy_c(o, s, core):
        at = band_of(core, s)
        return remote(lat.at[o, at], lat.at[o, at], send_c.at[o], recv_c.at[o], cfg=other)

    def sent_rows(o, count, sem):
        at = pl.ds(0, count)
        return remote(lat.at[o, at], lat.at[o, at], sem, recv_c.at[o], cfg=other)

    def half_of(o, core):
        at = pl.ds(aligned(core, half_rows), half_rows)
        return remote(lat.at[o, at], lat.at[o, at], send_c.at[o], recv_c.at[o], cfg=other)

    def first_p(d):
        return copy_p(z, d)

    def copy_p(o, d):
        return remote(pos.at[o], pos.at[o], send_p.at[o, up(d)], recv_p.at[o], seq=z + d)

    def first_t(d):
        return remote(text_kv.at[0], txt.at[z], send_t.at[z, up(d)], recv_t.at[z], seq=z + d)

    def copy_t(o, d):
        return remote(txt.at[o], txt.at[o], send_t.at[o, up(d)], recv_t.at[o], seq=z + d)

    def first_u():
        return remote(
            text_kv.at[0, :, :, cols_of(other)], txo.at[z], send_u.at[z], recv_u.at[z], cfg=other
        )

    def copy_u(o):
        return remote(txt.at[o, :, :, cols_of(other)], txo.at[o], send_u.at[o], recv_u.at[o], cfg=other)

    def copy_l(core):
        return remote(lens.at[core], lens.at[core], send_l.at[0], recv_l.at[0], cfg=other)

    lat_local.start()

    barrier = pltpu.get_barrier_semaphore()
    for d in (1, -1):

        @pl.when(inside(z + d))
        def _():
            pl.semaphore_signal(barrier, inc=1, device_id={"seq": z + d}, device_id_type=MESH)

    pl.semaphore_signal(barrier, inc=1, device_id={"cfg": other}, device_id_type=MESH)
    for t in range(1, ten_n):
        pl.semaphore_signal(
            barrier, inc=1, device_id={"tensor": (x + t) % ten_n}, device_id_type=MESH
        )

    def normalize(core, ten):
        spots = [strip_of(core, s, ten) for s in range(subs)]
        lanes = [slice(k * HEAD_DIM, (k + 1) * HEAD_DIM) for k in range(width // HEAD_DIM)]

        def mean_of(body):
            means = []
            for at in spots:
                total = body(at, lanes[0], len(means))
                for lane in lanes[1:]:
                    total = total + body(at, lane, len(means))
                means.append(jnp.sum(total, axis=-1, keepdims=True) * (1.0 / width))
            return means

        means = mean_of(lambda at, lane, n: lat[z, at, lane].astype(F32))

        def squared(at, lane, n):
            center = lat[z, at, lane].astype(F32) - means[n]
            return center * center

        inverses = [lax.rsqrt(power + 1e-06) for power in mean_of(squared)]
        for n, at in enumerate(spots):
            for lane in lanes:
                lat[z, at, lane] = (
                    (lat[z, at, lane].astype(F32) - means[n]) * inverses[n]
                ).astype(BF16)

    pos[z] = jnp.concatenate(
        [pos_in[...].astype(F32), jnp.zeros((16 - pos_in.shape[0], rows), F32)]
    ).astype(BF16)
    lens[c] = jnp.broadcast_to(lens_in[0:1, 0:1].astype(F32), lens.shape[1:])
    lat_local.wait()
    for j in range(3):
        w_local[j].start()
    txt_local.start()
    out_local.start()
    normalize(c, x)

    sides = jnp.where(z > 0, 1, 0) + jnp.where(z < seq_n - 1, 1, 0)
    pl.semaphore_wait(barrier, ten_n + sides)

    for d in (1, -1):

        @pl.when(inside(z + d))
        def _():
            first_p(d).start()
            for s in range(subs):
                copy_a(z, s, d).start()

    for j in range(3):
        w_copy[j].start()
    copy_l(c).start()
    first_u().start()

    @pl.loop(1, 2 * ten_n)
    def _(g):
        normalize(jnp.where(g < ten_n, c, other), (x + g) % ten_n)

    def pump_a(k, s):
        for d in (1, -1):
            o = z - d * k

            @pl.when(inside(o))
            def _():
                if s == 0:
                    copy_p(o, d).wait_recv()
                copy_a(o, s, d).wait_recv()

                @pl.when(inside(z + d))
                def _():
                    if s == 0:
                        copy_p(o, d).start()
                    copy_a(o, s, d).start()

    def pump_t(k):
        for d in (1, -1):
            o = z - d * k

            @pl.when(inside(o))
            def _():
                copy_t(o, d).wait_recv()

                @pl.when(inside(z + d))
                def _():
                    copy_t(o, d).start()

                copy_u(o).start()

    def start_b(o, s):
        for t in range(1, ten_n):
            copy_b(o, s, t).start()

    def end_b(o, s):
        for t in range(1, ten_n):
            arrived_b(o, s, t).wait_recv()
        copy_c(o, s, c).start()

    def front(k, p):
        @pl.when(k < seq_n)
        def _():
            for s in range(subs):
                if s * 4 // subs == p:
                    pump_a(k, s)
                    start_b(order(k), s)

    def back(k, p):
        @pl.when(k < seq_n)
        def _():
            for s in range(subs):
                if s * 4 // subs == p:
                    end_b(order(k), s)

    slots = 2 * tiles + 2

    def text_front(i, slot):
        last = seq_n - 1
        if slot == tiles:
            for d in (1, -1):

                @pl.when(jnp.logical_and(i == 1, inside(z + d)))
                def _():
                    first_t(d).start()

        if slot == 0 and last > 1:

            @pl.when(i == last)
            def _():
                pump_t(last - 1)

        if slot == tiles:

            @pl.when(jnp.logical_and(i > 1, i < last))
            def _():
                pump_t(i - 1)

        if slot == 2 * tiles - 1:

            @pl.when(i == last)
            def _():
                pump_t(last)

    def pump(i, slot):
        if slot == 0:
            front(i + 1, 2)
        if slot == min(2, 2 * tiles - 1):
            front(i + 1, 3)
        if slot == tiles:
            back(i + 1, 0)
        if slot == 2 * tiles - 1:
            back(i + 1, 1)
        if slot == 2 * tiles:
            back(i + 1, 2)
            front(i + 2, 0)
        if slot == slots - 1:
            back(i + 1, 3)
            front(i + 2, 1)
        text_front(i, slot)

    def project(j, t, b):
        at = pl.ds(t * tile, tile)
        return jnp.dot(
            mod[b * rows : (b + 1) * rows, :], wfull[j, :, at], preferred_element_type=F32
        )

    def finish(j, t, b, y):
        if j == 2:
            y = y.astype(BF16)
            for hh in range(per_tile):
                vbuf[b * heads + t * per_tile + hh] = y[:, hh * HEAD_DIM : (hh + 1) * HEAD_DIM]
            return
        swapped = jnp.dot(y.astype(BF16), mix[0, :tile, :tile], preferred_element_type=F32)
        square = jnp.dot((y * y).astype(BF16), mix[1, :tile, :tile], preferred_element_type=F32)
        inverse = lax.rsqrt(square + 1e-06)
        dest = kbuf if j == 1 else qbuf
        for hh in range(per_tile):
            at = slice(hh * HEAD_DIM, (hh + 1) * HEAD_DIM)
            turned = y[:, at] * tab[2 * j] + swapped[:, at] * tab[2 * j + 1]
            dest[b * heads + t * per_tile + hh] = (turned * inverse[:, at]).astype(BF16)

    def attend(span, first):
        ahead = {}
        for n in range(len(span) + 2):
            if n < len(span):
                h = span[n]
                ahead[n] = lax.dot_general(
                    qbuf[h], kbuf[h], (((1,), (1,)), ((), ())), preferred_element_type=F32
                )
            if n < 2:
                continue
            h = span[n - 2]
            expo = jnp.exp2(ahead.pop(n - 2))
            folded = expo[:, :HEAD_DIM]
            for k in range(1, rows // HEAD_DIM):
                folded = folded + expo[:, k * HEAD_DIM : (k + 1) * HEAD_DIM]
            mixed = jnp.dot(expo.astype(BF16), vbuf[h], preferred_element_type=F32)
            if first:
                lsum[h] = folded
                acc[h] = mixed
            else:
                lsum[h] += folded
                acc[h] += mixed

    def tables(o, first):
        place = lax.dot_general(
            pos[o], pick[...], (((0,), (0,)), ((), ())), preferred_element_type=F32
        )
        turns = place * rot[0:1, :]
        angle = (turns - jnp.floor(turns + 0.5)) * math.pi
        square = angle * angle
        low = angle * horner(SIN, square)
        cosine = 1.0 - 2.0 * low * low
        sine = 2.0 * low * horner(COS, square)
        for j in range(0 if first else 1, 2):
            strength = scale if j == 0 else 1.0
            tab[2 * j] = cosine * (gain_rows[j][0:1] * strength)
            tab[2 * j + 1] = sine * (gain_rows[j][1:2] * strength)

    swap_abs = jnp.abs(mix[0, :HEAD_DIM, :HEAD_DIM].astype(F32))
    gain_rows = []
    for j in range(2):
        own = gains[j : j + 1, :]
        column = jnp.sum(
            jnp.where(
                lax.broadcasted_iota(jnp.int32, (HEAD_DIM, HEAD_DIM), 0)
                == lax.broadcasted_iota(jnp.int32, (HEAD_DIM, HEAD_DIM), 1),
                own,
                0.0,
            ),
            axis=1,
            keepdims=True,
        )
        gain_rows.append(jnp.concatenate([own, jnp.sum(swap_abs * column, axis=0, keepdims=True)]))

    def modulate(o, core):
        @pl.loop(0, half_rows // STRIP, unroll=U_MOD)
        def _(r):
            start = aligned(core * (half_rows // STRIP) + r, STRIP)
            normed = lat[o, pl.ds(start, STRIP), :].astype(F32)
            for b in range(2):
                mod[pl.ds(pl.multiple_of(b * rows + start, STRIP), STRIP), :] = (
                    normed * (1.0 + modulation[1, b : b + 1, :]) + modulation[0, b : b + 1, :]
                ).astype(BF16)

    def step(i, first):
        o = order(i)
        tables(o, first)
        modulate(o, c)
        if not first:
            half_of(o, other).wait_recv()
        modulate(o, other)

        pending = None
        for j in range(0 if first else 1, 3):
            if first:
                w_local[j].wait()
                w_copy[j].wait_recv()
            for t in range(tiles):
                for b in range(2):
                    y = project(j, t, b)
                    if pending is not None:
                        finish(*pending)
                    pending = (j, t, b, y)
                if j > 0:
                    pump(i, (j - 1) * tiles + t)
                    continue
                if t == 0:
                    front(1, 0)
                if t == tiles - 1:
                    front(1, 1)
        finish(*pending)
        group = heads
        for g in range(2):
            attend(list(range(g * group, (g + 1) * group)), first)
            pump(i, 2 * tiles + g)

    step(0, True)

    @pl.loop(1, seq_n)
    def _(i):
        step(i, False)

    txt_local.wait()
    copy_l(other).wait_recv()

    @pl.loop(0, seq_n)
    def _(o):
        copy_u(o).wait_recv()

    text_rows = txt.shape[2]
    count = seq_n * text_rows

    def copy_o(core, t, own):
        to = (x + t) % ten_n
        branch = core if own == 0 else 1 - core
        at = pl.ds(aligned(branch, out_rows), out_rows)
        place = attf.at[core, to, at]
        return remote(place, place, send_o.at[t, own], recv_o.at[t, own], cfg=other)

    def text(t, own):
        to = (x + t) % ten_n
        here = pl.ds(aligned(to, out_rows), out_rows)
        branch = c if own == 0 else other
        source = txt if own == 0 else txo
        base = aligned(c, mine) if own == 0 else 0
        valid = lax.broadcasted_iota(jnp.int32, (1, count), 1).astype(F32) < lens[branch, 0:1, :]
        ahead = {}
        for n in range(heads + 2):
            if n < heads:
                src = pl.ds(pl.multiple_of(base + n * HEAD_DIM, HEAD_DIM), HEAD_DIM)
                raw = source[:, 0, :, src].reshape(count, HEAD_DIM).astype(F32)
                inverse = lax.rsqrt(jnp.mean(raw * raw, axis=-1, keepdims=True) + 1e-06)
                keys = (raw * inverse * gains[1:2, :]).astype(BF16)
                ahead[n] = lax.dot_general(
                    qbuf[branch * heads + n, here, :],
                    keys,
                    (((1,), (1,)), ((), ())),
                    preferred_element_type=F32,
                )
            if n < 2:
                continue
            h = n - 2
            row = branch * heads + h
            src = pl.ds(pl.multiple_of(base + h * HEAD_DIM, HEAD_DIM), HEAD_DIM)
            values = source[:, 1, :, src].reshape(count, HEAD_DIM)
            expo = jnp.where(valid, jnp.exp2(ahead.pop(h)), 0.0)
            total = jnp.sum(lsum[row, here, :], axis=-1, keepdims=True) + jnp.sum(
                expo, axis=-1, keepdims=True
            )
            mixed = acc[row, here, :] + jnp.dot(
                expo.astype(BF16), values, preferred_element_type=F32
            )
            attf[
                c, to, pl.ds(aligned(branch, out_rows), out_rows), h * HEAD_DIM : (h + 1) * HEAD_DIM
            ] = (mixed * (1.0 / total)).astype(BF16)
        copy_o(c, t, own).start()

    out_tile = 256 if out_cols % 256 == 0 else 128
    out_tiles = out_cols // out_tile

    def copy_r(t, k):
        return remote(
            part.at[t, k], got.at[t, k], send_r.at[t - 1], recv_r.at[t - 1, k], tensor=(x + t) % ten_n
        )

    strength = guide[0:1, 0:1]

    def out_block(t, k):
        to = (x + t) % ten_n
        at = pl.ds(aligned(k, out_tile), out_tile)
        y = jnp.dot(attf[0, to], wout[0:mine, at], preferred_element_type=F32)
        y = y + jnp.dot(attf[1, to], wout[mine : 2 * mine, at], preferred_element_type=F32)
        at_gate = pl.ds(pl.multiple_of(c * out_cols + k * out_tile, out_tile), out_tile)
        return (
            y[:out_rows] * (strength * modulation[2, 0:1, at_gate])
            + y[out_rows:] * ((1.0 - strength) * modulation[2, 1:2, at_gate])
        )

    turn = list(range(1, ten_n)) + [0]
    text(turn[0], 0)
    text(turn[0], 1)
    out_local.wait()
    for n, t in enumerate(turn):
        if n + 1 < ten_n:
            text(turn[n + 1], 0)
        copy_o(other, t, 0).wait_recv()
        copy_o(other, t, 1).wait_recv()
        if t > 0:

            @pl.loop(0, out_tiles)
            def _(k):
                part[t, k] = out_block(t, k).astype(BF16)
                copy_r(t, k).start()

        else:
            for k in range(out_tiles):
                part[t, k] = out_block(t, k).astype(BF16)
        if n + 1 < ten_n:
            text(turn[n + 1], 1)

    for j in range(3):
        w_copy[j].wait_send()
    copy_l(c).wait_send()
    for t in range(ten_n):
        for own in range(2):
            copy_o(c, t, own).wait_send()

    @pl.loop(0, seq_n)
    def _(o):
        copy_u(o).wait_send()

        @pl.when(o != z)
        def _():
            for t in range(1, ten_n):
                sent_rows(o, subs * STRIP, send_b.at[o, t - 1]).wait_send()
            sent_rows(o, half_rows, send_c.at[o]).wait_send()

        for d in (1, -1):
            ahead = jnp.logical_or(o == z, d * (z - o) > 0)

            @pl.when(jnp.logical_and(ahead, inside(z + d)))
            def _():
                copy_p(o, d).wait_send()
                copy_t(o, d).wait_send()
                sent_rows(o, subs * STRIP, send_a.at[o, up(d)]).wait_send()

    def emit(k):
        return pltpu.make_async_copy(
            part.at[0, k], out.at[:, pl.ds(k * out_tile, out_tile)], loc.at[8 + k]
        )

    for k in range(out_tiles):
        total = part[0, k].astype(F32)
        for t in range(1, ten_n):
            copy_r(t, k).wait_recv()
            total = total + got[t, k].astype(F32)
        part[0, k] = total.astype(BF16)
        emit(k).start()
    for t in range(1, ten_n):
        remote(
            part.at[t], got.at[t], send_r.at[t - 1], recv_r.at[t - 1, 0], tensor=(x + t) % ten_n
        ).wait_send()
    for k in range(out_tiles):
        emit(k).wait()


def local(
    seq_n, ten_n, latent, positions, text_kv, text_len, modulation, w_qkv, norm_gains, w_out, guidance
):
    rows, width = latent.shape
    mine = w_qkv.shape[2] // 2
    heads = mine // HEAD_DIM
    text_dev = text_kv.shape[2]
    out_rows = rows // ten_n
    out_cols = w_out.shape[1]
    out_tile = 256 if out_cols % 256 == 0 else 128
    out_tiles = out_cols // out_tile
    subs = rows // (2 * ten_n * STRIP)
    any_space = pl.BlockSpec(memory_space=pl.ANY)
    vmem = pl.BlockSpec(memory_space=pltpu.VMEM)
    dma = pltpu.SemaphoreType.DMA
    return pl.pallas_call(
        functools.partial(kernel, seq_n, ten_n),
        out_shape=jax.ShapeDtypeStruct((out_rows, out_cols), BF16),
        in_specs=[
            any_space,
            vmem,
            any_space,
            vmem,
            vmem,
            any_space,
            vmem,
            any_space,
            vmem,
            vmem,
            vmem,
            vmem,
        ],
        out_specs=any_space,
        scratch_shapes=[
            pltpu.VMEM((seq_n, rows, width), BF16),
            pltpu.VMEM((seq_n, 16, rows), BF16),
            pltpu.VMEM((seq_n, 2, text_dev, 2 * mine), BF16),
            pltpu.VMEM((seq_n, 2, text_dev, mine), BF16),
            pltpu.VMEM((2, 8, seq_n * text_dev), F32),
            pltpu.VMEM((3, width, mine), BF16),
            pltpu.VMEM(w_out.shape, BF16),
            pltpu.VMEM((2 * rows, width), BF16),
            pltpu.VMEM((4, rows, HEAD_DIM), F32),
            pltpu.VMEM((2 * heads, rows, HEAD_DIM), BF16),
            pltpu.VMEM((2 * heads, rows, HEAD_DIM), BF16),
            pltpu.VMEM((2 * heads, rows, HEAD_DIM), BF16),
            pltpu.VMEM((2 * heads, rows, HEAD_DIM), F32),
            pltpu.VMEM((2 * heads, rows, HEAD_DIM), F32),
            pltpu.VMEM((2, ten_n, 2 * out_rows, mine), BF16),
            pltpu.VMEM((ten_n, out_tiles, out_rows, out_tile), BF16),
            pltpu.VMEM((ten_n, out_tiles, out_rows, out_tile), BF16),
            dma((seq_n, 2)),
            dma((seq_n, subs)),
            dma((seq_n, max(ten_n - 1, 1))),
            dma((seq_n, subs, max(ten_n - 1, 1))),
            dma((seq_n,)),
            dma((seq_n,)),
            dma((seq_n, 2)),
            dma((seq_n,)),
            dma((seq_n, 2)),
            dma((seq_n,)),
            dma((seq_n,)),
            dma((seq_n,)),
            dma((3,)),
            dma((3,)),
            dma((1,)),
            dma((1,)),
            dma((ten_n, 2)),
            dma((ten_n, 2)),
            dma((max(ten_n - 1, 1),)),
            dma((max(ten_n - 1, 1), out_tiles)),
            dma((8 + out_tiles,)),
        ],
        compiler_params=pltpu.CompilerParams(
            collective_id=0, has_side_effects=True, vmem_limit_bytes=64 * 1024 * 1024 - 65536
        ),
    )(
        latent,
        positions,
        text_kv,
        text_len.reshape(1, 1),
        modulation,
        w_qkv,
        norm_gains,
        w_out,
        guidance.reshape(1, 1),
        jnp.asarray(ROT_ROWS),
        jnp.asarray(ROT_PICK, BF16),
        jnp.asarray(MIX, BF16),
    )


def solution(mesh):
    placed = (
        P(("groups", "seq"), None),
        P(None, ("groups", "seq")),
        P("cfg", None, ("groups", "seq"), "tensor"),
        P(("groups", "cfg")),
        P(None, "groups", None),
        P(None, "cfg", "tensor"),
        P(),
        P("tensor", "cfg"),
        P("groups"),
    )
    return jax.shard_map(
        functools.partial(local, mesh.shape["seq"], mesh.shape["tensor"]),
        mesh=mesh,
        in_specs=placed,
        out_specs=P(("groups", "seq", "tensor"), "cfg"),
        check_vma=False,
    )
```
